512 devices in a mesh: blk: 8 (over x, z_hi), wide: 64 (over z_lo, y, core).
Axes of the slice: x: 4, y: 8, z: 8 (z_hi: 2, z_lo: 4; z = z_hi * 4 + z_lo), core: 2. Of those that a mesh axis runs over, the one named last changes fastest.
Arguments:
- volume: float32 [8, 2, 2048, 896], P('blk', None, 'wide'), may hold values from -1.6 to 1.6
- path_lengths: float32 [8, 8, 2], replicated, may hold values from 0.5 to 2
- probe: float32 [2, 128, 128], replicated, may hold values from -6 to 6
- measured: bfloat16 [8, 64, 14, 128, 128], P('blk', 'wide'), may hold values from 0.19921875 to 3
- jitter: int32 [2, 8, 64, 14], P(None, 'blk', 'wide'), may hold values from 0 to 15
- step_sizes: float32 [8], replicated, may hold values from 0.02 to 0.2
Outputs:
- new_volume: float32 [8, 2, 2048, 896], P('blk', None, 'wide')
- misfit: float32 [], replicated
The draws below stay inside these ranges and needn't reach their ends.
All inputs are finite; a program needn't handle non-finite values.
Results may differ from the reference program's by a relative error of at most 0.0003.
Values sent between devices are 32-bit elements; how exact they have to be, the bound alone decides.
A program may use at most 64 MiB of HBM per device.

```python
import math
import jax
import jax.numpy as jnp
from jax import lax

LAYERS = 2
ROWS_DEV = 32
COLS = 896
PATCH = 128
CSTEP = 64
JIT = 16
PCOLS = 14
HEIGHT = 2048
N_BLK = 8
N_WIDE = 64


def with_ends(drawn, stream_key, least, largest):
    extent = drawn.shape
    spot = [jax.random.randint(jax.random.fold_in(stream_key, axis), (), 0, extent[axis]) for axis in range(len(extent))]
    drawn = drawn.at[tuple(spot)].set(least)
    longest = extent.index(max(extent))
    spot[longest] = (spot[longest] + 1) % extent[longest]
    return drawn.at[tuple(spot)].set(largest)


def shard_levels(rng, dims, pieces, smallest, top_value):
    loudness, own = 1.0, jax.random.fold_in(rng, 6)
    for dim, shards_of in pieces:
        draws = jnp.exp(jax.random.uniform(jax.random.fold_in(own, dim), (shards_of,), jnp.float32, smallest / len(pieces), top_value / len(pieces)))
        loudness = loudness * jnp.repeat(draws, dims[dim] // shards_of).reshape([-1 if axis == dim else 1 for axis in range(len(dims))])
    return loudness


def noise(key, dims, scale, bound, shards=(), kind=jnp.bfloat16):
    drawn = jax.random.normal(key, dims, jnp.float32) * scale
    if len(shards) > 0:
        drawn = shard_levels(key, dims, shards, -0.22, 0.18) * drawn
    return jnp.clip(drawn, min=-bound, max=bound).astype(kind)


def setup_inputs(seed: int = 0) -> dict:
    streams_of = jax.random.split(jax.random.key(seed), 7)
    return {
        "volume": noise(streams_of[0], (N_BLK, LAYERS, HEIGHT, COLS), 0.2, 1.6, ((0, 8), (2, 64)), jnp.float32),
        "path_lengths": jnp.clip(jnp.exp(jax.random.uniform(streams_of[1], (N_BLK, N_BLK, LAYERS), jnp.float32, math.log(0.5), math.log(2.0))), 0.5, 2.0),
        "probe": noise(streams_of[2], (2, PATCH, PATCH), 1.0, 6.0, (), jnp.float32),
        "measured": jnp.clip(jnp.exp(math.log(3.0) - 2.7119641 * jax.random.uniform(streams_of[3], (N_BLK, N_WIDE, PCOLS, PATCH, PATCH), jnp.float32) ** shard_levels(streams_of[3], (N_BLK, N_WIDE, PCOLS, PATCH, PATCH), ((0, 8), (1, 64)), -0.2, 0.2)), 0.19921875, 3.0).astype(jnp.bfloat16),
        "jitter": with_ends(jax.random.randint(streams_of[4], (2, N_BLK, N_WIDE, PCOLS), 0, JIT), jax.random.fold_in(streams_of[4], 1), 0, JIT - 1).astype(jnp.int32),
        "step_sizes": jnp.clip(jnp.exp(jax.random.uniform(streams_of[5], (N_BLK,), jnp.float32, math.log(0.02), math.log(0.2))), 0.02, 0.2),
    }


highest = lax.Precision.HIGHEST
floor_value = 0.25

def dft_tables(length):
    grid = jnp.arange(length, dtype=jnp.int32)
    product = grid[:, None] * grid[None, :] % length
    angles = product.astype(jnp.float32) * (2.0 * math.pi / length)
    factor = 1.0 / math.sqrt(length)
    return (jnp.cos(angles) * factor, -jnp.sin(angles) * factor)

def left_apply(table, batch):
    return jnp.einsum('jk,bkl->bjl', table, batch, precision=highest)

def right_apply(batch, table):
    return jnp.einsum('bjk,kl->bjl', batch, table, precision=highest)

def transform(real_in, imag_in, cos_table, sin_table):
    mid_real = left_apply(cos_table, real_in) - left_apply(sin_table, imag_in)
    mid_imag = left_apply(cos_table, imag_in) + left_apply(sin_table, real_in)
    out_real = right_apply(mid_real, cos_table) - right_apply(mid_imag, sin_table)
    out_imag = right_apply(mid_real, sin_table) + right_apply(mid_imag, cos_table)
    return (out_real, out_imag)

def strip_update(strip_real, strip_imaginary, probe, measured, jitter_rows, jitter_cols, row_corner, column_corner):
    patch_len = probe.shape[-1]
    number = measured.shape[0]
    cos_table, sin_table = dft_tables(patch_len)
    starts_row = (row_corner + jitter_rows).astype(jnp.int32)
    starts_col = (column_corner + CSTEP * jnp.arange(number, dtype=jnp.int32) + jitter_cols).astype(jnp.int32)

    def window(image, top, left):
        return lax.dynamic_slice(image, (top, left), (patch_len, patch_len))
    pick = jax.vmap(window, in_axes=(None, 0, 0))
    obj_real = pick(strip_real, starts_row, starts_col)
    obj_imag = pick(strip_imaginary, starts_row, starts_col)
    probe_real = probe[0]
    probe_imag = probe[1]
    wave_real = probe_real * obj_real - probe_imag * obj_imag
    wave_imag = probe_real * obj_imag + probe_imag * obj_real
    far_real, far_imag = transform(wave_real, wave_imag, cos_table, sin_table)
    modulus = jnp.sqrt(far_real * far_real + far_imag * far_imag)
    target = measured.astype(jnp.float32)
    error = modulus - target
    partial_misfit = jnp.sum(error * error)
    ratio = target / jnp.maximum(modulus, floor_value)
    back_real, back_imag = transform(ratio * far_real, ratio * far_imag, cos_table, -sin_table)
    diff_real = back_real - wave_real
    diff_imag = back_imag - wave_imag
    corr_real = probe_real * diff_real + probe_imag * diff_imag
    corr_imag = probe_real * diff_imag - probe_imag * diff_real

    def place(position, sums):
        acc_real, acc_imag = sums
        top = starts_row[position]
        left = starts_col[position]
        acc_real = lax.dynamic_update_slice(acc_real, window(acc_real, top, left) + corr_real[position], (top, left))
        acc_imag = lax.dynamic_update_slice(acc_imag, window(acc_imag, top, left) + corr_imag[position], (top, left))
        return (acc_real, acc_imag)
    zeros = jnp.zeros(strip_real.shape, strip_real.dtype)
    acc_real, acc_imag = lax.fori_loop(0, number, place, (zeros, zeros))
    return (acc_real, acc_imag, partial_misfit)

def reference(volume, path_lengths, probe, measured, jitter, step_sizes):
    projections = jnp.einsum('asl,slhc->ahc', path_lengths, volume, precision=highest)
    margin = PATCH // 2
    row_corner = ROWS_DEV // 4
    column_corner = PATCH // 4 - ROWS_DEV // 4
    height = ROWS_DEV * N_WIDE
    band_rows = 5 * ROWS_DEV
    gradients = []
    total = jnp.zeros((), jnp.float32)
    for angle in range(N_BLK):
        phase = projections[angle]
        obj_real = jnp.pad(jnp.cos(phase), ((2 * ROWS_DEV, 2 * ROWS_DEV), (margin, margin)))
        obj_imag = jnp.pad(jnp.sin(phase), ((2 * ROWS_DEV, 2 * ROWS_DEV), (margin, margin)))
        width_all = obj_real.shape[1]

        def row_step(carry, input_arrays):
            acc_real, acc_imag, running = carry
            strip_index, recorded_row, shaken_rows, shaken_columns = input_arrays
            top = (strip_index * ROWS_DEV).astype(jnp.int32)
            zero_col = jnp.zeros((), jnp.int32)
            strip_real = lax.dynamic_slice(obj_real, (top, zero_col), (band_rows, width_all))
            strip_imaginary = lax.dynamic_slice(obj_imag, (top, zero_col), (band_rows, width_all))
            portion_real, portion_imaginary, part = strip_update(strip_real, strip_imaginary, probe, recorded_row, shaken_rows, shaken_columns, row_corner, column_corner)
            acc_real = lax.dynamic_update_slice(acc_real, lax.dynamic_slice(acc_real, (top, zero_col), (band_rows, width_all)) + portion_real, (top, zero_col))
            acc_imag = lax.dynamic_update_slice(acc_imag, lax.dynamic_slice(acc_imag, (top, zero_col), (band_rows, width_all)) + portion_imaginary, (top, zero_col))
            return ((acc_real, acc_imag, running + part), None)
        input_arrays = (jnp.arange(N_WIDE, dtype=jnp.int32), measured[angle], jitter[0, angle], jitter[1, angle])
        start = (jnp.zeros(obj_real.shape, jnp.float32), jnp.zeros(obj_real.shape, jnp.float32), jnp.zeros((), jnp.float32))
        (acc_real, acc_imag, part), unused = lax.scan(row_step, start, input_arrays)
        total = total + part
        inner_r = slice(2 * ROWS_DEV, 2 * ROWS_DEV + height)
        inner_c = slice(margin, margin + COLS)
        gradients.append(obj_real[inner_r, inner_c] * acc_imag[inner_r, inner_c] - obj_imag[inner_r, inner_c] * acc_real[inner_r, inner_c])
    stacked = jnp.stack(gradients, 0)
    coeffs = step_sizes[:, None, None] * path_lengths
    update = jnp.einsum('asl,ahc->slhc', coeffs, stacked, precision=highest)
    return (volume - update, total)
```

```python
import functools

import jax
import jax.numpy as jnp
import ml_dtypes
import numpy as np
from jax import lax
from jax.experimental import pallas as pl
from jax.experimental.pallas import tpu as pltpu
from jax.sharding import PartitionSpec as P

ROWS = 32
COLS = 896
PATCH = 128
PCOLS = 14
N_BLK = 8
N_WIDE = 64
TILES = COLS // 128
FRAME = 144
TOP = 56
CHUNK = 32
F32 = jnp.float32
BF16 = jnp.bfloat16


def dft_tables():
    n = np.arange(PATCH)
    angle = (n[:, None] * n[None, :] % PATCH) * (2 * np.pi / PATCH)
    c = np.cos(angle) / np.sqrt(float(PATCH))
    s = -np.sin(angle) / np.sqrt(float(PATCH))
    out = []
    for t in (np.block([[c, s], [-s, c]]), np.block([[c, -s], [s, c]])):
        t = t.astype(np.float32)
        hi = t.astype(ml_dtypes.bfloat16)
        out += [hi, (t - hi.astype(np.float32)).astype(ml_dtypes.bfloat16)]
    return np.stack(out)


def cos_sin(x):
    k = jnp.floor(x * np.float32(2 / np.pi) + np.float32(0.5))
    r = x - k * np.float32(1.5703125)
    r = r - k * np.float32(4.837512969970703125e-4)
    r = r - k * np.float32(7.54978995489188216e-8)
    z = r * r
    sn = ((np.float32(-1.9515295891e-4) * z + np.float32(8.3321608736e-3)) * z - np.float32(1.6666654611e-1)) * z * r + r
    cs = ((np.float32(2.443315711809948e-5) * z - np.float32(1.388731625493765e-3)) * z + np.float32(4.166664568298827e-2)) * z * z
    cs = cs - np.float32(0.5) * z + np.float32(1.0)
    q = k.astype(jnp.int32)
    swap = (q & 1) == 1
    co = jnp.where(swap, sn, cs)
    si = jnp.where(swap, cs, sn)
    co = jnp.where(((q + 1) & 2) == 2, -co, co)
    si = jnp.where((q & 2) == 2, -si, si)
    return co, si


def halves(x):
    hi = x.astype(BF16)
    return hi, (x - hi.astype(F32)).astype(BF16)


def mm(a, b):
    return jnp.dot(a, b, preferred_element_type=F32)


def row_chunks():
    return [pl.ds(r, CHUNK) for r in range(0, PATCH, CHUNK)]


def mid_kernel(phase, probe, measured, jitter, tables, grad, misfit, cosf, sinf, acc, probe2, wave, xs, vs, err):
    w = lax.axis_index("wide")
    probe2[:, :PATCH] = probe[...]
    probe2[:, PATCH:] = probe[...]
    first = TOP - ROWS * w
    for r in range(0, FRAME, 16):
        row = lax.broadcasted_iota(jnp.int32, (16, COLS), 0) + r
        inside = (row >= first) & (row < first + ROWS * N_WIDE)
        co, si = cos_sin(phase[r : r + 16, :])
        co = jnp.where(inside, co, 0.0)
        si = jnp.where(inside, si, 0.0)
        for t in range(TILES):
            cosf[t + 1, r : r + 16, :] = co[:, t * 128 : t * 128 + 128]
            sinf[t + 1, r : r + 16, :] = si[:, t * 128 : t * 128 + 128]
    for t in (0, TILES + 1):
        cosf[t] = jnp.zeros((FRAME, 128), F32)
        sinf[t] = jnp.zeros((FRAME, 128), F32)
    acc[...] = jnp.zeros(acc.shape, F32)
    err[...] = jnp.zeros(err.shape, F32)

    def masks(pair, p):
        j = 2 * pair + p
        jr = jitter[0, j]
        s = (24 if p else 88) + jitter[1, j]
        lane = lax.broadcasted_iota(jnp.int32, (CHUNK, PATCH), 1) >= s
        row = lax.broadcasted_iota(jnp.int32, (16, PATCH), 0) >= jr
        return j, jr, s, lane, row

    def step(pair, slot):
        t1h, t1l, t2h, t2l = (tables[i] for i in range(4))
        for p in range(2):
            j, jr, s, lane, row = masks(pair, p)
            t = pair + p
            for c in range(0, PATCH, CHUNK):
                def pick(ref):
                    a = ref[t, c : c + CHUNK, :]
                    b = ref[t + 1, c : c + CHUNK, :]
                    if c == 0:
                        a0 = jnp.where(row, a[:16], ref[t, PATCH:, :])
                        b0 = jnp.where(row, b[:16], ref[t + 1, PATCH:, :])
                        a = jnp.concatenate([a0, a[16:]], 0)
                        b = jnp.concatenate([b0, b[16:]], 0)
                    return jnp.where(lane, a, b)
                o_r, o_i = pick(cosf), pick(sinf)
                at = pl.ds(PATCH - jr + c, CHUNK)
                p_r = pltpu.roll(probe2[0, at, :], s, 1)
                p_i = pltpu.roll(probe2[1, at, :], s, 1)
                w_r = p_r * o_r - p_i * o_i
                w_i = p_r * o_i + p_i * o_r
                wave[slot, p, 0, c : c + CHUNK, :] = w_r
                wave[slot, p, 1, c : c + CHUNK, :] = w_i
                put_rows(slot, p, c, w_r, w_i)
        right_to_cols(slot, t1h, t1l)
        y = left(slot, t2h, t2l)
        e = err[...]
        for p in range(2):
            j = 2 * pair + p
            for c in range(0, PATCH, CHUNK):
                f_r = y[c : c + CHUNK, p * 128 : p * 128 + 128]
                f_i = y[PATCH + c : PATCH + c + CHUNK, p * 128 : p * 128 + 128]
                m2 = f_r * f_r + f_i * f_i
                target = measured[j, c : c + CHUNK, :].astype(F32)
                d = jnp.sqrt(m2) - target
                d2 = d * d
                for k in range(0, CHUNK, 8):
                    e = e + d2[k : k + 8]
                ratio = target * lax.rsqrt(jnp.maximum(m2, 0.0625))
                put_rows(slot, p, c, ratio * f_r, ratio * f_i)
        err[...] = e
        right_to_cols(slot, t2h, t2l)
        y = left(slot, t1h, t1l)
        for p in range(2):
            j, jr, s, lane, row = masks(pair, p)
            t = pair + p
            for c in range(0, PATCH, CHUNK):
                b_r = y[c : c + CHUNK, p * 128 : p * 128 + 128]
                b_i = y[PATCH + c : PATCH + c + CHUNK, p * 128 : p * 128 + 128]
                g = wave[slot, p, 0, c : c + CHUNK, :] * b_i - wave[slot, p, 1, c : c + CHUNK, :] * b_r
                for tile, part in ((t, jnp.where(lane, g, 0.0)), (t + 1, jnp.where(lane, 0.0, g))):
                    if c == 0:
                        acc[tile, PATCH:, :] += jnp.where(row, 0.0, part[:16])
                        part = jnp.concatenate([jnp.where(row, part[:16], 0.0), part[16:]], 0)
                    acc[tile, c : c + CHUNK, :] += part

    def put_rows(slot, p, c, a, b):
        at = slice(p * PATCH + c, p * PATCH + c + CHUNK)
        for k, x in enumerate((a, b)):
            hi, lo = halves(x)
            xs[slot, at, k * 128 : k * 128 + 128] = hi
            xs[slot, at, 256 + k * 128 : 256 + k * 128 + 128] = lo

    def right_to_cols(slot, th, tl):
        x = xs[slot]
        u = mm(jnp.concatenate([x, x[:, :256]], 1), jnp.concatenate([th, th, tl], 0))
        for p in range(2):
            for k in range(2):
                for c in range(0, PATCH, CHUNK):
                    hi, lo = halves(u[p * PATCH + c : p * PATCH + c + CHUNK, k * 128 : k * 128 + 128])
                    vs[slot, k * PATCH + c : k * PATCH + c + CHUNK, p * 128 : p * 128 + 128] = hi
                    vs[slot, 256 + k * PATCH + c : 256 + k * PATCH + c + CHUNK, p * 128 : p * 128 + 128] = lo

    def left(slot, th, tl):
        v = vs[slot]
        return mm(jnp.concatenate([th, th, tl], 1), jnp.concatenate([v, v[:256]], 0))

    SLOTS = xs.shape[0]
    if SLOTS == PCOLS // 2:
        for pair in range(PCOLS // 2):
            step(pair, pair)
    else:
        def loop(i, carry):
            step(i, 0)
            return carry
        lax.fori_loop(0, PCOLS // 2, loop, 0)
    for t in range(TILES):
        grad[:, t * 128 : t * 128 + 128] = acc[t + 1]
    misfit[...] = err[...]


def middle(phase, probe, measured, jitter, slots=7):
    vm = pl.BlockSpec(memory_space=pltpu.VMEM)
    return pl.pallas_call(
        mid_kernel,
        out_shape=(jax.ShapeDtypeStruct((FRAME, COLS), F32), jax.ShapeDtypeStruct((8, 128), F32)),
        in_specs=[vm, vm, vm, pl.BlockSpec(memory_space=pltpu.SMEM), vm],
        out_specs=(vm, vm),
        scratch_shapes=[
            pltpu.VMEM((TILES + 2, FRAME, 128), F32),
            pltpu.VMEM((TILES + 2, FRAME, 128), F32),
            pltpu.VMEM((TILES + 2, FRAME, 128), F32),
            pltpu.VMEM((2, 2 * PATCH, PATCH), F32),
            pltpu.VMEM((slots, 2, 2, PATCH, PATCH), F32),
            pltpu.VMEM((slots, 2 * PATCH, 512), BF16),
            pltpu.VMEM((slots, 512, 2 * PATCH), BF16),
            pltpu.VMEM((8, 128), F32),
        ],
        name="middle",
    )(phase, probe, measured, jitter, jnp.asarray(dft_tables()))


def shifted(x, by):
    pairs = [(i, i + by) for i in range(N_WIDE) if 0 <= i + by < N_WIDE]
    return lax.ppermute(x, "wide", pairs)


def body(volume, path_lengths, probe, measured, jitter, step_sizes):
    group = lax.axis_index("blk")
    slab = volume[0]
    own = lax.dynamic_index_in_dim(path_lengths, group, 1, keepdims=False)
    terms = own[:, 0, None, None] * slab[0] + own[:, 1, None, None] * slab[1]
    proj = jnp.sum(lax.all_to_all(terms, "blk", 0, 0, tiled=True), 0)
    frame = jnp.concatenate(
        [shifted(proj[8:], 2), shifted(proj, 1), proj, shifted(proj, -1), shifted(proj[:24], -2)], 0
    )
    part, err = middle(frame, probe, measured[0, 0], jitter[:, 0, 0])
    grad = part[56:88]
    grad = grad + shifted(part[24:56], -1) + shifted(part[88:120], 1)
    grad = grad + jnp.pad(shifted(part[:24], -2), ((8, 0), (0, 0))) + jnp.pad(shifted(part[120:], 2), ((0, 8), (0, 0)))
    total = lax.psum(jnp.sum(err), ("blk", "wide"))
    every = lax.all_to_all(jnp.broadcast_to(grad[None], (N_BLK, ROWS, COLS)), "blk", 0, 0, tiled=True)
    coeffs = step_sizes[:, None] * own
    update = jnp.sum(coeffs[:, :, None, None] * every[:, None], 0)
    return (slab - update)[None], total


def solution(mesh):
    in_specs = (
        P("blk", None, "wide", None),
        P(),
        P(),
        P("blk", "wide", None, None, None),
        P(None, "blk", "wide", None),
        P(),
    )
    out_specs = (P("blk", None, "wide", None), P())
    return jax.shard_map(body, mesh=mesh, in_specs=in_specs, out_specs=out_specs, check_vma=False)
```

```python
import functools

import jax
import jax.numpy as jnp
import ml_dtypes
import numpy as np
from jax import lax
from jax.experimental import pallas as pl
from jax.experimental.pallas import tpu as pltpu
from jax.sharding import PartitionSpec as P

ROWS = 32
COLS = 896
PATCH = 128
PCOLS = 14
N_BLK = 8
N_WIDE = 64
MESH = pl.DeviceIdType.MESH
TILES = COLS // 128
FRAME = 144
TOP = 56
CHUNK = 32
F32 = jnp.float32
BF16 = jnp.bfloat16


def dft_tables():
    n = np.arange(PATCH)
    angle = (n[:, None] * n[None, :] % PATCH) * (2 * np.pi / PATCH)
    c = np.cos(angle) / np.sqrt(float(PATCH))
    s = -np.sin(angle) / np.sqrt(float(PATCH))
    out = []
    for t in (np.block([[c, s], [-s, c]]), np.block([[c, -s], [s, c]])):
        t = t.astype(np.float32)
        hi = t.astype(ml_dtypes.bfloat16)
        out += [hi, (t - hi.astype(np.float32)).astype(ml_dtypes.bfloat16)]
    return np.stack(out)


def cos_sin(x):
    k = jnp.floor(x * np.float32(2 / np.pi) + np.float32(0.5))
    r = x - k * np.float32(1.5703125)
    r = r - k * np.float32(4.837512969970703125e-4)
    r = r - k * np.float32(7.54978995489188216e-8)
    z = r * r
    sn = ((np.float32(-1.9515295891e-4) * z + np.float32(8.3321608736e-3)) * z - np.float32(1.6666654611e-1)) * z * r + r
    cs = ((np.float32(2.443315711809948e-5) * z - np.float32(1.388731625493765e-3)) * z + np.float32(4.166664568298827e-2)) * z * z
    cs = cs - np.float32(0.5) * z + np.float32(1.0)
    q = k.astype(jnp.int32)
    swap = (q & 1) == 1
    co = jnp.where(swap, sn, cs)
    si = jnp.where(swap, cs, sn)
    co = jnp.where(((q + 1) & 2) == 2, -co, co)
    si = jnp.where((q & 2) == 2, -si, si)
    return co, si


def halves(x):
    hi = x.astype(BF16)
    return hi, (x - hi.astype(F32)).astype(BF16)


def mm(a, b):
    return jnp.dot(a, b, preferred_element_type=F32)


def row_chunks():
    return [pl.ds(r, CHUNK) for r in range(0, PATCH, CHUNK)]


def fused_kernel(
    volume, paths, steps, probe, measured, jitter, tables,
    out, total,
    xa, zs, zr, phase, cosf, sinf, acc, back, pair_g, ga, probe2, wave, xs, vs, err, mbuf,
    send_sems, recv_sems,
):
    g = lax.axis_index("blk")
    w = lax.axis_index("wide")
    x, zh = g // 2, g % 2
    zl, y, core = w // 16, (w // 2) % 8, w % 2
    z = zh * 4 + zl

    def device(x_, y_, z_, core_):
        return (x_ * 2 + z_ // 4, (z_ % 4) * 16 + y_ * 2 + core_)

    x_up, x_down, x_far = (x + 1) % 4, (x + 3) % 4, (x + 2) % 4
    ring = [(x_up * 2 + zh, w), (x_down * 2 + zh, w), (x_far * 2 + zh, w)]
    across = (g + 1 - 2 * zh, w)
    groups = (
        (z, [device(x, y, (z + k) % 8, core) for k in range(1, 8)]),
        (y, [device(x, (y + k) % 8, z, core) for k in range(1, 8)]),
        (x * 2 + core, [device((x + k // 2) % 4, y, z, (core + k) % 2) for k in range(1, 8)]),
    )
    near = [(-1, w >= 1), (1, w < N_WIDE - 1), (-2, w >= 2), (2, w < N_WIDE - 2)]

    counter = [0]
    pending = []

    def copy(src, dst, device_id, when=None):
        k = counter[0]
        counter[0] += 1
        c = pltpu.make_async_remote_copy(
            src_ref=src, dst_ref=dst, send_sem=send_sems.at[k], recv_sem=recv_sems.at[k],
            device_id=device_id, device_id_type=MESH,
        )
        return c

    def guarded(cond, f):
        if cond is None:
            f()
        else:
            pl.when(cond)(f)

    def start(c, cond=None):
        guarded(cond, c.start)
        pending.append((c, cond))

    def arrive(c, cond=None):
        guarded(cond, c.wait_recv)

    tile = [slice(c * 128, c * 128 + 128) for c in range(TILES)]
    hop = [[copy(volume.at[:, :, tile[c]], xa.at[k, c], ring[k]) for k in range(3)] for c in range(TILES)]
    cross = [copy(zs.at[c], zr.at[c], across) for c in range(TILES)]
    rows_sent = {-1: (56, 32, 88), 1: (56, 32, 24), -2: (56, 24, 120), 2: (64, 24, 0)}
    halo = [
        [copy(phase.at[c, pl.ds(rows_sent[d][0], rows_sent[d][1]), :], phase.at[c, pl.ds(rows_sent[d][2], rows_sent[d][1]), :],
              (g, jnp.clip(w + d, 0, N_WIDE - 1))) for d, _ in near]
        for c in range(TILES)
    ]
    rows_back = {-1: (24, 32, 0), 1: (88, 32, 32), -2: (0, 24, 64), 2: (120, 24, 88)}
    ret = [
        [copy(acc.at[c + 1, pl.ds(rows_back[d][0], rows_back[d][1]), :], back.at[c, pl.ds(rows_back[d][2], rows_back[d][1]), :],
              (g, jnp.clip(w + d, 0, N_WIDE - 1))) for d, _ in near]
        for c in range(TILES)
    ]
    gcross = [copy(pair_g.at[c, 0], pair_g.at[c, 1], across) for c in range(TILES)]
    ghop = [[[copy(pair_g.at[c, h], ga.at[k, c, h], ring[k]) for k in range(3)] for h in range(2)] for c in range(TILES)]
    sums = [[copy(mbuf.at[s, groups[s][0]], mbuf.at[s, groups[s][0]], p) for p in groups[s][1]] for s in range(3)]

    barrier = pltpu.get_barrier_semaphore()
    for _, members in groups:
        for p in members:
            pl.semaphore_signal(barrier, inc=1, device_id=p, device_id_type=MESH)
    for d, cond in near:
        @pl.when(cond)
        def _():
            pl.semaphore_signal(barrier, inc=1, device_id=(g, jnp.clip(w + d, 0, N_WIDE - 1)), device_id_type=MESH)

    init = jax.named_scope('init')
    init.__enter__()
    probe2[:, :PATCH] = probe[...]
    probe2[:, PATCH:] = probe[...]
    for t in (0, TILES + 1):
        cosf[t] = jnp.zeros((FRAME, 128), F32)
        sinf[t] = jnp.zeros((FRAME, 128), F32)
    acc[...] = jnp.zeros(acc.shape, F32)
    err[...] = jnp.zeros(err.shape, F32)

    init.__exit__(None, None, None)
    neighbours = sum(cond.astype(jnp.int32) for _, cond in near)
    with jax.named_scope('wait'):
        pl.semaphore_wait(barrier, 21 + neighbours)

    slabs = [g, x_down * 2 + zh, x_up * 2 + zh, x_far * 2 + zh]

    def stage_b(c):
        for k in range(3):
            arrive(hop[c][k])
        blocks = [(volume[l, :, tile[c]], xa[0, c, l], xa[1, c, l], xa[2, c, l]) for l in range(2)]

        def term(angle):
            s = jnp.zeros((ROWS, 128), F32)
            for l in range(2):
                for k in range(4):
                    s = s + paths[angle, l, slabs[k]] * blocks[l][k]
            return s

        zs[c] = term(g + 1 - 2 * zh)
        start(cross[c])
        phase[c, TOP : TOP + ROWS, :] = term(g)

    def stage_c(c):
        arrive(cross[c])
        phase[c, TOP : TOP + ROWS, :] = phase[c, TOP : TOP + ROWS, :] + zr[c]
        for k, (d, cond) in enumerate(near):
            start(halo[c][k], cond)

    first = TOP - ROWS * w

    def stage_d(c):
        for k in (1, 0, 3, 2):
            d = near[k][0]
            arrive(halo[c][k], {1: w >= 1, -1: w < N_WIDE - 1, 2: w >= 2, -2: w < N_WIDE - 2}[d])
        for r in range(0, FRAME, 24):
            row = lax.broadcasted_iota(jnp.int32, (24, 128), 0) + r
            inside = (row >= first) & (row < first + ROWS * N_WIDE)
            co, si = cos_sin(jnp.where(inside, phase[c, r : r + 24, :], 0.0))
            cosf[c + 1, r : r + 24, :] = jnp.where(inside, co, 0.0)
            sinf[c + 1, r : r + 24, :] = jnp.where(inside, si, 0.0)

    def masks(pair, p):
        j = 2 * pair + p
        jr = jitter[0, j]
        s = (24 if p else 88) + jitter[1, j]
        lane = lax.broadcasted_iota(jnp.int32, (CHUNK, PATCH), 1) >= s
        row = lax.broadcasted_iota(jnp.int32, (16, PATCH), 0) >= jr
        return j, jr, s, lane, row

    def step(pair, slot):
        t1h, t1l, t2h, t2l = (tables[i] for i in range(4))
        for p in range(2):
            j, jr, s, lane, row = masks(pair, p)
            t = pair + p
            for c in range(0, PATCH, CHUNK):
                def pick(ref):
                    a = ref[t, c : c + CHUNK, :]
                    b = ref[t + 1, c : c + CHUNK, :]
                    if c == 0:
                        a0 = jnp.where(row, a[:16], ref[t, PATCH:, :])
                        b0 = jnp.where(row, b[:16], ref[t + 1, PATCH:, :])
                        a = jnp.concatenate([a0, a[16:]], 0)
                        b = jnp.concatenate([b0, b[16:]], 0)
                    return jnp.where(lane, a, b)
                o_r, o_i = pick(cosf), pick(sinf)
                at = pl.ds(PATCH - jr + c, CHUNK)
                p_r = pltpu.roll(probe2[0, at, :], s, 1)
                p_i = pltpu.roll(probe2[1, at, :], s, 1)
                w_r = p_r * o_r - p_i * o_i
                w_i = p_r * o_i + p_i * o_r
                wave[slot, p, 0, c : c + CHUNK, :] = w_r
                wave[slot, p, 1, c : c + CHUNK, :] = w_i
                put_rows(slot, p, c, w_r, w_i)
        right_to_cols(slot, t1h, t1l)
        y = left(slot, t2h, t2l)
        e = err[...]
        for p in range(2):
            j = 2 * pair + p
            for c in range(0, PATCH, CHUNK):
                f_r = y[c : c + CHUNK, p * 128 : p * 128 + 128]
                f_i = y[PATCH + c : PATCH + c + CHUNK, p * 128 : p * 128 + 128]
                m2 = f_r * f_r + f_i * f_i
                target = measured[j, c : c + CHUNK, :].astype(F32)
                d = jnp.sqrt(m2) - target
                d2 = d * d
                for k in range(0, CHUNK, 8):
                    e = e + d2[k : k + 8]
                ratio = target * lax.rsqrt(jnp.maximum(m2, 0.0625))
                put_rows(slot, p, c, ratio * f_r, ratio * f_i)
        err[...] = e
        right_to_cols(slot, t2h, t2l)
        y = left(slot, t1h, t1l)
        for p in range(2):
            j, jr, s, lane, row = masks(pair, p)
            t = pair + p
            for c in range(0, PATCH, CHUNK):
                b_r = y[c : c + CHUNK, p * 128 : p * 128 + 128]
                b_i = y[PATCH + c : PATCH + c + CHUNK, p * 128 : p * 128 + 128]
                g = wave[slot, p, 0, c : c + CHUNK, :] * b_i - wave[slot, p, 1, c : c + CHUNK, :] * b_r
                for tile, part in ((t, jnp.where(lane, g, 0.0)), (t + 1, jnp.where(lane, 0.0, g))):
                    if c == 0:
                        acc[tile, PATCH:, :] += jnp.where(row, 0.0, part[:16])
                        part = jnp.concatenate([jnp.where(row, part[:16], 0.0), part[16:]], 0)
                    acc[tile, c : c + CHUNK, :] += part

    def put_rows(slot, p, c, a, b):
        at = slice(p * PATCH + c, p * PATCH + c + CHUNK)
        for k, x in enumerate((a, b)):
            hi, lo = halves(x)
            xs[slot, at, k * 128 : k * 128 + 128] = hi
            xs[slot, at, 256 + k * 128 : 256 + k * 128 + 128] = lo

    def right_to_cols(slot, th, tl):
        x = xs[slot]
        u = mm(jnp.concatenate([x, x[:, :256]], 1), jnp.concatenate([th, th, tl], 0))
        for p in range(2):
            for k in range(2):
                for c in range(0, PATCH, CHUNK):
                    hi, lo = halves(u[p * PATCH + c : p * PATCH + c + CHUNK, k * 128 : k * 128 + 128])
                    vs[slot, k * PATCH + c : k * PATCH + c + CHUNK, p * 128 : p * 128 + 128] = hi
                    vs[slot, 256 + k * PATCH + c : 256 + k * PATCH + c + CHUNK, p * 128 : p * 128 + 128] = lo

    def left(slot, th, tl):
        v = vs[slot]
        return mm(jnp.concatenate([th, th, tl], 1), jnp.concatenate([v, v[:256]], 0))

    def stage_e(pair):
        step(pair, pair % 2)

    def stage_f(c):
        for k, (d, cond) in enumerate(near):
            start(ret[c][k], cond)

    def stage_g(c):
        s = acc[c + 1, TOP : TOP + ROWS, :]
        pair_g[c, 0] = s
        for k, (d, cond) in enumerate(near):
            ok = {1: w >= 1, -1: w < N_WIDE - 1, 2: w >= 2, -2: w < N_WIDE - 2}[d]
            lo, n, at = {-1: (0, 32, 0), 1: (0, 32, 32), -2: (8, 24, 64), 2: (0, 24, 88)}[d]

            @pl.when(ok)
            def _():
                ret[c][k].wait_recv()
                pair_g[c, 0, lo : lo + n, :] = pair_g[c, 0, lo : lo + n, :] + back[c, at : at + n, :]

        start(gcross[c])
        for k in range(3):
            start(ghop[c][0][k])

    def stage_h(c):
        arrive(gcross[c])
        for k in range(3):
            start(ghop[c][1][k])

    angles = [g, g + 1 - 2 * zh, x_down * 2 + zh, x_down * 2 + 1 - zh, x_up * 2 + zh, x_up * 2 + 1 - zh, x_far * 2 + zh, x_far * 2 + 1 - zh]

    def stage_j(c):
        for k in range(3):
            arrive(ghop[c][0][k])
            arrive(ghop[c][1][k])
        grads = [pair_g[c, 0], pair_g[c, 1], *(ga[k, c, h] for k in range(3) for h in range(2))]
        for l in range(2):
            s = jnp.zeros((ROWS, 128), F32)
            for a, gr in zip(angles, grads):
                s = s + (steps[a] * paths[a, l, g]) * gr
            out[l, :, tile[c]] = s

    def misfit_send(s, value):
        mbuf[s, pl.ds(groups[s][0], 1)] = value[None]
        for c in sums[s]:
            start(c)

    def misfit_take(s):
        for c in sums[s]:
            arrive(c)
        v = mbuf[s, 0]
        for k in range(1, 8):
            v = v + mbuf[s, k]
        return v

    for c in range(TILES):
        for k in range(3):
            start(hop[c][k])

    def stage_m(c):
        value = misfit_take(c - 1) if c else err[...]
        if c < 3:
            misfit_send(c, value)
        else:
            total[0] = jnp.sum(value)

    stages = dict(zip("BCDEFGHJM", (stage_b, stage_c, stage_d, stage_e, stage_f, stage_g, stage_h, stage_j, stage_m)))
    for name, c in order():
        with jax.named_scope(f"{name}{c}"):
            stages[name](c)
    for c, cond in pending:
        guarded(cond, c.wait_send)


DUE = dict(
    B=(3.2, 1.4), C=(8.5, 1.4), D=(11.3, 1.4), E=(12.75, 1.55), F=(15.85, 1.55),
    G=(19.0, 1.55), H=(24.5, 1.55), J=(28.1, 1.55), M=(23.7, 4.5),
)


def order():
    due = []
    for name, (begin, gap) in DUE.items():
        for c in range(4 if name == "M" else TILES):
            last = TILES - 2 if name == "F" else TILES
            due.append((begin + gap * min(c, last), name, c))
    return [(name, c) for _, name, c in sorted(due)]


def fused(volume, paths, steps, probe, measured, jitter):
    vm = pl.BlockSpec(memory_space=pltpu.VMEM)
    sm = pl.BlockSpec(memory_space=pltpu.SMEM)
    copies = TILES * 19 + 21
    grid = pltpu.VMEM((TILES + 2, FRAME, 128), F32)
    return pl.pallas_call(
        fused_kernel,
        out_shape=(jax.ShapeDtypeStruct((2, ROWS, COLS), F32), jax.ShapeDtypeStruct((1,), F32)),
        in_specs=[vm, sm, sm, vm, vm, sm, vm],
        out_specs=(vm, sm),
        scratch_shapes=[
            pltpu.VMEM((3, TILES, 2, ROWS, 128), F32),
            pltpu.VMEM((TILES, ROWS, 128), F32),
            pltpu.VMEM((TILES, ROWS, 128), F32),
            pltpu.VMEM((TILES, FRAME, 128), F32),
            grid, grid, grid,
            pltpu.VMEM((TILES, 112, 128), F32),
            pltpu.VMEM((TILES, 2, ROWS, 128), F32),
            pltpu.VMEM((3, TILES, 2, ROWS, 128), F32),
            pltpu.VMEM((2, 2 * PATCH, PATCH), F32),
            pltpu.VMEM((2, 2, 2, PATCH, PATCH), F32),
            pltpu.VMEM((2, 2 * PATCH, 512), BF16),
            pltpu.VMEM((2, 512, 2 * PATCH), BF16),
            pltpu.VMEM((8, 128), F32),
            pltpu.VMEM((3, 8, 8, 128), F32),
            pltpu.SemaphoreType.DMA((copies,)),
            pltpu.SemaphoreType.DMA((copies,)),
        ],
        compiler_params=pltpu.CompilerParams(collective_id=0, has_side_effects=True),
        name="fused",
    )(volume, paths, steps, probe, measured, jitter, jnp.asarray(dft_tables()))


def body(volume, path_lengths, probe, measured, jitter, step_sizes):
    paths = jnp.transpose(path_lengths, (0, 2, 1))
    update, total = fused(volume[0], paths, step_sizes, probe, measured[0, 0], jitter[:, 0, 0])
    return volume - update[None], total[0]


def solution(mesh):
    in_specs = (
        P("blk", None, "wide", None),
        P(),
        P(),
        P("blk", "wide", None, None, None),
        P(None, "blk", "wide", None),
        P(),
    )
    out_specs = (P("blk", None, "wide", None), P())
    return jax.shard_map(body, mesh=mesh, in_specs=in_specs, out_specs=out_specs, check_vma=False)
```

```python
import functools

import jax
import jax.numpy as jnp
import ml_dtypes
import numpy as np
from jax import lax
from jax.experimental import pallas as pl
from jax.experimental.pallas import tpu as pltpu
from jax.sharding import PartitionSpec as P

ROWS = 32
COLS = 896
PATCH = 128
PCOLS = 14
N_BLK = 8
N_WIDE = 64
MESH = pl.DeviceIdType.MESH
TILES = COLS // 128
FRAME = 144
TOP = 56
CHUNK = 32
F32 = jnp.float32
BF16 = jnp.bfloat16


def dft_tables():
    n = np.arange(PATCH)
    angle = (n[:, None] * n[None, :] % PATCH) * (2 * np.pi / PATCH)
    c = np.cos(angle) / np.sqrt(float(PATCH))
    s = -np.sin(angle) / np.sqrt(float(PATCH))
    out = []
    for t in (np.block([[c, s], [-s, c]]), np.block([[c, -s], [s, c]])):
        t = t.astype(np.float32)
        hi = t.astype(ml_dtypes.bfloat16)
        out += [hi, (t - hi.astype(np.float32)).astype(ml_dtypes.bfloat16)]
    return np.stack(out)


def cos_sin(x):
    k = jnp.floor(x * np.float32(2 / np.pi) + np.float32(0.5))
    r = x - k * np.float32(1.5703125)
    r = r - k * np.float32(4.837512969970703125e-4)
    r = r - k * np.float32(7.54978995489188216e-8)
    z = r * r
    sn = ((np.float32(-1.9515295891e-4) * z + np.float32(8.3321608736e-3)) * z - np.float32(1.6666654611e-1)) * z * r + r
    cs = ((np.float32(2.443315711809948e-5) * z - np.float32(1.388731625493765e-3)) * z + np.float32(4.166664568298827e-2)) * z * z
    cs = cs - np.float32(0.5) * z + np.float32(1.0)
    q = k.astype(jnp.int32)
    swap = (q & 1) == 1
    co = jnp.where(swap, sn, cs)
    si = jnp.where(swap, cs, sn)
    co = jnp.where(((q + 1) & 2) == 2, -co, co)
    si = jnp.where((q & 2) == 2, -si, si)
    return co, si


def halves(x):
    hi = x.astype(BF16)
    return hi, (x - hi.astype(F32)).astype(BF16)


def mm(a, b):
    return jnp.dot(a, b, preferred_element_type=F32)


def row_chunks():
    return [pl.ds(r, CHUNK) for r in range(0, PATCH, CHUNK)]


def fused_kernel(
    volume_in, paths_in, steps_in, probe_in, measured_in, jitter_in, tables_in,
    out, total,
    volume, measured, tables, paths, steps, jitter, load_sems,
    xa, zs, zr, phase, cosf, sinf, acc, back, pair_g, ga, probe2, wave, xs, vs, err, mbuf,
    send_sems, recv_sems,
):
    g = lax.axis_index("blk")
    w = lax.axis_index("wide")
    x, zh = g // 2, g % 2
    zl, y, core = w // 16, (w // 2) % 8, w % 2
    z = zh * 4 + zl

    def device(x_, y_, z_, core_):
        return (x_ * 2 + z_ // 4, (z_ % 4) * 16 + y_ * 2 + core_)

    x_up, x_down, x_far = (x + 1) % 4, (x + 3) % 4, (x + 2) % 4
    ring = [(x_up * 2 + zh, w), (x_down * 2 + zh, w), (x_far * 2 + zh, w)]
    across = (g + 1 - 2 * zh, w)
    groups = (
        (y, [device(x, (y + k) % 8, z, core) for k in range(1, 8)]),
        (z, [device(x, y, (z + k) % 8, core) for k in range(1, 8)]),
        (x * 2 + core, [device((x + k // 2) % 4, y, z, (core + k) % 2) for k in range(1, 8)]),
    )
    near = [(-1, w >= 1), (1, w < N_WIDE - 1), (-2, w >= 2), (2, w < N_WIDE - 2)]

    counter = [0]
    pending = []

    def copy(src, dst, device_id, when=None):
        k = counter[0]
        counter[0] += 1
        c = pltpu.make_async_remote_copy(
            src_ref=src, dst_ref=dst, send_sem=send_sems.at[k], recv_sem=recv_sems.at[k],
            device_id=device_id, device_id_type=MESH,
        )
        return c

    def guarded(cond, f):
        if cond is None:
            f()
        else:
            pl.when(cond)(f)

    def start(c, cond=None):
        guarded(cond, c.start)
        pending.append((c, cond))

    def arrive(c, cond=None):
        guarded(cond, c.wait_recv)

    tile = [slice(c * 128, c * 128 + 128) for c in range(TILES)]
    hop = [[copy(volume.at[:, :, tile[c]], xa.at[k, c], ring[k]) for k in range(3)] for c in range(TILES)]
    cross = [copy(zs.at[c], zr.at[c], across) for c in range(TILES)]
    rows_sent = {-1: (56, 32, 88), 1: (56, 32, 24), -2: (56, 24, 120), 2: (64, 24, 0)}
    halo = [
        [copy(phase.at[c, pl.ds(rows_sent[d][0], rows_sent[d][1]), :], phase.at[c, pl.ds(rows_sent[d][2], rows_sent[d][1]), :],
              (g, jnp.clip(w + d, 0, N_WIDE - 1))) for d, _ in near]
        for c in range(TILES)
    ]
    rows_back = {-1: (24, 32, 0), 1: (88, 32, 32), -2: (0, 24, 64), 2: (120, 24, 88)}
    ret = [
        [copy(acc.at[c + 1, pl.ds(rows_back[d][0], rows_back[d][1]), :], back.at[c, pl.ds(rows_back[d][2], rows_back[d][1]), :],
              (g, jnp.clip(w + d, 0, N_WIDE - 1))) for d, _ in near]
        for c in range(TILES)
    ]
    gcross = [copy(pair_g.at[c, 0], pair_g.at[c, 1], across) for c in range(TILES)]
    ghop = [[[copy(pair_g.at[c, h], ga.at[k, c, h], ring[k]) for k in range(3)] for h in range(2)] for c in range(TILES)]
    sums = [[copy(mbuf.at[s, groups[s][0]], mbuf.at[s, groups[s][0]], p) for p in groups[s][1]] for s in range(3)]

    loads = [
        pltpu.make_async_copy(src, dst, load_sems.at[k])
        for k, (src, dst) in enumerate((
            (volume_in, volume), (probe_in, probe2.at[:, pl.ds(0, PATCH)]), (probe_in, probe2.at[:, pl.ds(PATCH, PATCH)]),
            (paths_in, paths), (steps_in, steps), (jitter_in, jitter), (measured_in, measured), (tables_in, tables),
        ))
    ]
    barrier = pltpu.get_barrier_semaphore()
    for _, members in groups:
        for p in members:
            pl.semaphore_signal(barrier, inc=1, device_id=p, device_id_type=MESH)
    for d, cond in near:
        @pl.when(cond)
        def _():
            pl.semaphore_signal(barrier, inc=1, device_id=(g, jnp.clip(w + d, 0, N_WIDE - 1)), device_id_type=MESH)

    for c in loads:
        c.start()
    for t in (0, TILES + 1):
        cosf[t] = jnp.zeros((FRAME, 128), F32)
        sinf[t] = jnp.zeros((FRAME, 128), F32)
    acc[...] = jnp.zeros(acc.shape, F32)
    err[...] = jnp.zeros(err.shape, F32)

    neighbours = sum(cond.astype(jnp.int32) for _, cond in near)
    loads[0].wait()
    with jax.named_scope("wait"):
        pl.semaphore_wait(barrier, 21 + neighbours)
    for c in range(TILES):
        for k in range(3):
            start(hop[c][k])
    for c in loads[1:]:
        c.wait()

    slabs = [g, x_down * 2 + zh, x_up * 2 + zh, x_far * 2 + zh]

    def stage_b(c):
        for k in range(3):
            arrive(hop[c][k])
        blocks = [(volume[l, :, tile[c]], xa[0, c, l], xa[1, c, l], xa[2, c, l]) for l in range(2)]

        def term(angle):
            s = jnp.zeros((ROWS, 128), F32)
            for l in range(2):
                for k in range(4):
                    s = s + paths[angle, l, slabs[k]] * blocks[l][k]
            return s

        zs[c] = term(g + 1 - 2 * zh)
        start(cross[c])
        phase[c, TOP : TOP + ROWS, :] = term(g)

    def stage_c(c):
        arrive(cross[c])
        phase[c, TOP : TOP + ROWS, :] = phase[c, TOP : TOP + ROWS, :] + zr[c]
        for k, (d, cond) in enumerate(near):
            start(halo[c][k], cond)

    first = TOP - ROWS * w

    def stage_d(c):
        for k in (1, 0, 3, 2):
            d = near[k][0]
            arrive(halo[c][k], {1: w >= 1, -1: w < N_WIDE - 1, 2: w >= 2, -2: w < N_WIDE - 2}[d])
        for r in range(0, FRAME, 24):
            row = lax.broadcasted_iota(jnp.int32, (24, 128), 0) + r
            inside = (row >= first) & (row < first + ROWS * N_WIDE)
            co, si = cos_sin(jnp.where(inside, phase[c, r : r + 24, :], 0.0))
            cosf[c + 1, r : r + 24, :] = jnp.where(inside, co, 0.0)
            sinf[c + 1, r : r + 24, :] = jnp.where(inside, si, 0.0)

    def masks(pair, p):
        j = 2 * pair + p
        jr = jitter[0, j]
        s = (24 if p else 88) + jitter[1, j]
        lane = lax.broadcasted_iota(jnp.int32, (CHUNK, PATCH), 1) >= s
        row = lax.broadcasted_iota(jnp.int32, (16, PATCH), 0) >= jr
        return j, jr, s, lane, row

    def put_rows(slot, p, c, a, b):
        at = slice(p * PATCH + c, p * PATCH + c + CHUNK)
        for k, x in enumerate((a, b)):
            hi, lo = halves(x)
            xs[slot, at, k * 128 : k * 128 + 128] = hi
            xs[slot, at, 256 + k * 128 : 256 + k * 128 + 128] = lo

    def right(slot, th, tl):
        x = xs[slot]
        return mm(jnp.concatenate([x, x[:, :256]], 1), jnp.concatenate([th, th, tl], 0))

    def to_cols(slot, u):
        for p in range(2):
            for k in range(2):
                for c in range(0, PATCH, CHUNK):
                    hi, lo = halves(u[p * PATCH + c : p * PATCH + c + CHUNK, k * 128 : k * 128 + 128])
                    vs[slot, k * PATCH + c : k * PATCH + c + CHUNK, p * 128 : p * 128 + 128] = hi
                    vs[slot, 256 + k * PATCH + c : 256 + k * PATCH + c + CHUNK, p * 128 : p * 128 + 128] = lo

    def left(slot, th, tl):
        v = vs[slot]
        return mm(jnp.concatenate([th, th, tl], 1), jnp.concatenate([v, v[:256]], 0))

    def waves(pair, slot):
        for p in range(2):
            j, jr, s, lane, row = masks(pair, p)
            t = pair + p
            for c in range(0, PATCH, CHUNK):
                def pick(ref):
                    a = ref[t, c : c + CHUNK, :]
                    b = ref[t + 1, c : c + CHUNK, :]
                    if c == 0:
                        a0 = jnp.where(row, a[:16], ref[t, PATCH:, :])
                        b0 = jnp.where(row, b[:16], ref[t + 1, PATCH:, :])
                        a = jnp.concatenate([a0, a[16:]], 0)
                        b = jnp.concatenate([b0, b[16:]], 0)
                    return jnp.where(lane, a, b)
                o_r, o_i = pick(cosf), pick(sinf)
                at = pl.ds(PATCH - jr + c, CHUNK)
                p_r = pltpu.roll(probe2[0, at, :], s, 1)
                p_i = pltpu.roll(probe2[1, at, :], s, 1)
                w_r = p_r * o_r - p_i * o_i
                w_i = p_r * o_i + p_i * o_r
                wave[slot, p, 0, c : c + CHUNK, :] = w_r
                wave[slot, p, 1, c : c + CHUNK, :] = w_i
                put_rows(slot, p, c, w_r, w_i)
    def pointwise(pair, slot, y):
        e = err[...]
        for p in range(2):
            j = 2 * pair + p
            for c in range(0, PATCH, CHUNK):
                f_r = y[c : c + CHUNK, p * 128 : p * 128 + 128]
                f_i = y[PATCH + c : PATCH + c + CHUNK, p * 128 : p * 128 + 128]
                m2 = f_r * f_r + f_i * f_i
                target = measured[j, c : c + CHUNK, :].astype(F32)
                d = jnp.sqrt(m2) - target
                d2 = d * d
                for k in range(0, CHUNK, 8):
                    e = e + d2[k : k + 8]
                ratio = target * lax.rsqrt(jnp.maximum(m2, 0.0625))
                put_rows(2 + slot, p, c, ratio * f_r, ratio * f_i)
        err[...] = e
    def accumulate(pair, slot, y):
        for p in range(2):
            j, jr, s, lane, row = masks(pair, p)
            t = pair + p
            for c in range(0, PATCH, CHUNK):
                b_r = y[c : c + CHUNK, p * 128 : p * 128 + 128]
                b_i = y[PATCH + c : PATCH + c + CHUNK, p * 128 : p * 128 + 128]
                g = wave[slot, p, 0, c : c + CHUNK, :] * b_i - wave[slot, p, 1, c : c + CHUNK, :] * b_r
                for tile, part in ((t, jnp.where(lane, g, 0.0)), (t + 1, jnp.where(lane, 0.0, g))):
                    if c == 0:
                        acc[tile, PATCH:, :] += jnp.where(row, 0.0, part[:16])
                        part = jnp.concatenate([jnp.where(row, part[:16], 0.0), part[16:]], 0)
                    acc[tile, c : c + CHUNK, :] += part

    def stage_e(i):
        t1h, t1l, t2h, t2l = (tables[k] for k in range(4))
        ahead, behind = i < PCOLS // 2, i > 0
        if behind:
            u2 = right(2 + (i - 1) % 2, t2h, t2l)
        if ahead:
            waves(i, i % 2)
            u1 = right(i % 2, t1h, t1l)
        if behind:
            to_cols(1, u2)
            y2 = left(1, t1h, t1l)
        if ahead:
            to_cols(0, u1)
            y1 = left(0, t2h, t2l)
        if behind:
            accumulate(i - 1, (i - 1) % 2, y2)
        if ahead:
            pointwise(i, i % 2, y1)

    def stage_f(c):
        for k, (d, cond) in enumerate(near):
            start(ret[c][k], cond)

    def stage_g(c):
        s = acc[c + 1, TOP : TOP + ROWS, :]
        pair_g[c, 0] = s
        for k, (d, cond) in enumerate(near):
            ok = {1: w >= 1, -1: w < N_WIDE - 1, 2: w >= 2, -2: w < N_WIDE - 2}[d]
            lo, n, at = {-1: (0, 32, 0), 1: (0, 32, 32), -2: (8, 24, 64), 2: (0, 24, 88)}[d]

            @pl.when(ok)
            def _():
                ret[c][k].wait_recv()
                pair_g[c, 0, lo : lo + n, :] = pair_g[c, 0, lo : lo + n, :] + back[c, at : at + n, :]

        start(gcross[c])
        for k in range(3):
            start(ghop[c][0][k])

    def stage_h(c):
        arrive(gcross[c])
        for k in range(3):
            start(ghop[c][1][k])

    angles = [g, g + 1 - 2 * zh, x_down * 2 + zh, x_down * 2 + 1 - zh, x_up * 2 + zh, x_up * 2 + 1 - zh, x_far * 2 + zh, x_far * 2 + 1 - zh]

    def stage_j(c):
        for k in range(3):
            arrive(ghop[c][0][k])
            arrive(ghop[c][1][k])
        grads = [pair_g[c, 0], pair_g[c, 1], *(ga[k, c, h] for k in range(3) for h in range(2))]
        for l in range(2):
            s = jnp.zeros((ROWS, 128), F32)
            for a, gr in zip(angles, grads):
                s = s + (steps[a] * paths[a, l, g]) * gr
            out[l, :, tile[c]] = s

    def misfit_send(s, value):
        mbuf[s, pl.ds(groups[s][0], 1)] = value[None]
        for c in sums[s]:
            start(c)

    def misfit_take(s):
        for c in sums[s]:
            arrive(c)
        v = mbuf[s, 0]
        for k in range(1, 8):
            v = v + mbuf[s, k]
        return v

    def stage_m(c):
        value = misfit_take(c - 1) if c else err[...]
        if c < 3:
            misfit_send(c, value)
        else:
            total[0] = jnp.sum(value)

    stages = dict(zip("BCDEFGHJM", (stage_b, stage_c, stage_d, stage_e, stage_f, stage_g, stage_h, stage_j, stage_m)))
    for name, c in order():
        with jax.named_scope(f"{name}{c}"):
            stages[name](c)
    for c, cond in pending:
        guarded(cond, c.wait_send)


STEP = 1.0


def order():
    tiles = range(TILES)
    due = [(2.2 + 1.4 * c, "B", c) for c in tiles] + [(8.1 + 1.4 * c, "C", c) for c in tiles]
    ready = [11.6 + 1.4 * c for c in tiles]
    due += [(t, "D", c) for c, t in enumerate(ready)]
    done, now = [], 0.0
    for i in range(TILES + 1):
        now = max(now, ready[min(i + 1, TILES - 1)] + 0.01)
        due.append((now, "E", i))
        now += STEP
        done.append(now - 0.01)
    for c in tiles:
        t = done[min(c + 2, TILES)]
        due += [(t, "F", c), (t + 3.8 - 0.15 * c, "G", c), (t + 9.3 - 0.15 * c, "H", c), (t + 13.5 - 0.15 * c, "J", c)]
    due += [(done[TILES - 1] - 0.001 + 4.6 * c, "M", c) for c in range(4)]
    return [(name, c) for _, name, c in sorted(due)]


def fused(volume, paths, steps, probe, measured, jitter):
    vm = pl.BlockSpec(memory_space=pltpu.VMEM)
    hbm = pl.BlockSpec(memory_space=pl.ANY)
    sm = pl.BlockSpec(memory_space=pltpu.SMEM)
    copies = TILES * 19 + 21
    grid = pltpu.VMEM((TILES + 2, FRAME, 128), F32)
    return pl.pallas_call(
        fused_kernel,
        out_shape=(pltpu.VMEM((2, ROWS, COLS), F32), jax.ShapeDtypeStruct((1,), F32)),
        in_specs=[hbm] * 7,
        out_specs=(vm, sm),
        scratch_shapes=[
            pltpu.VMEM((2, ROWS, COLS), F32),
            pltpu.VMEM((PCOLS, PATCH, PATCH), BF16),
            pltpu.VMEM((4, 2 * PATCH, 2 * PATCH), BF16),
            pltpu.SMEM((8, 2, 8), F32),
            pltpu.SMEM((8,), F32),
            pltpu.SMEM((2, PCOLS), jnp.int32),
            pltpu.SemaphoreType.DMA((8,)),
            pltpu.VMEM((3, TILES, 2, ROWS, 128), F32),
            pltpu.VMEM((TILES, ROWS, 128), F32),
            pltpu.VMEM((TILES, ROWS, 128), F32),
            pltpu.VMEM((TILES, FRAME, 128), F32),
            grid, grid, grid,
            pltpu.VMEM((TILES, 112, 128), F32),
            pltpu.VMEM((TILES, 2, ROWS, 128), F32),
            pltpu.VMEM((3, TILES, 2, ROWS, 128), F32),
            pltpu.VMEM((2, 2 * PATCH, PATCH), F32),
            pltpu.VMEM((2, 2, 2, PATCH, PATCH), F32),
            pltpu.VMEM((4, 2 * PATCH, 512), BF16),
            pltpu.VMEM((2, 512, 2 * PATCH), BF16),
            pltpu.VMEM((8, 128), F32),
            pltpu.VMEM((3, 8, 8, 128), F32),
            pltpu.SemaphoreType.DMA((copies,)),
            pltpu.SemaphoreType.DMA((copies,)),
        ],
        compiler_params=pltpu.CompilerParams(collective_id=0, has_side_effects=True),
        name="fused",
    )(volume, paths, steps, probe, measured, jitter, jnp.asarray(dft_tables()))


def body(volume, path_lengths, probe, measured, jitter, step_sizes):
    paths = jnp.transpose(path_lengths, (0, 2, 1))
    update, total = fused(volume[0], paths, step_sizes, probe, measured[0, 0], jitter[:, 0, 0])
    return volume - update[None], total[0]


def solution(mesh):
    in_specs = (
        P("blk", None, "wide", None),
        P(),
        P(),
        P("blk", "wide", None, None, None),
        P(None, "blk", "wide", None),
        P(),
    )
    out_specs = (P("blk", None, "wide", None), P())
    return jax.shard_map(body, mesh=mesh, in_specs=in_specs, out_specs=out_specs, check_vma=False)
```

```python
import functools

import jax
import jax.numpy as jnp
import ml_dtypes
import numpy as np
from jax import lax
from jax.experimental import pallas as pl
from jax.experimental.pallas import tpu as pltpu
from jax.sharding import PartitionSpec as P

ROWS = 32
COLS = 896
PATCH = 128
PCOLS = 14
N_BLK = 8
N_WIDE = 64
MESH = pl.DeviceIdType.MESH
TILES = COLS // 128
FRAME = 144
TOP = 56
CHUNK = 32
F32 = jnp.float32
BF16 = jnp.bfloat16


def dft_tables():
    n = np.arange(PATCH)
    angle = (n[:, None] * n[None, :] % PATCH) * (2 * np.pi / PATCH)
    c = np.cos(angle) / np.sqrt(float(PATCH))
    s = -np.sin(angle) / np.sqrt(float(PATCH))
    out = []
    for t in (np.block([[c, s], [-s, c]]), np.block([[c, -s], [s, c]])):
        t = t.astype(np.float32)
        hi = t.astype(ml_dtypes.bfloat16)
        out += [hi, (t - hi.astype(np.float32)).astype(ml_dtypes.bfloat16)]
    return np.stack(out)


def cos_sin(x):
    k = jnp.floor(x * np.float32(2 / np.pi) + np.float32(0.5))
    r = x - k * np.float32(1.5703125)
    r = r - k * np.float32(4.837512969970703125e-4)
    r = r - k * np.float32(7.54978995489188216e-8)
    z = r * r
    sn = ((np.float32(-1.9515295891e-4) * z + np.float32(8.3321608736e-3)) * z - np.float32(1.6666654611e-1)) * z * r + r
    cs = ((np.float32(2.443315711809948e-5) * z - np.float32(1.388731625493765e-3)) * z + np.float32(4.166664568298827e-2)) * z * z
    cs = cs - np.float32(0.5) * z + np.float32(1.0)
    q = k.astype(jnp.int32)
    swap = (q & 1) == 1
    co = jnp.where(swap, sn, cs)
    si = jnp.where(swap, cs, sn)
    co = jnp.where(((q + 1) & 2) == 2, -co, co)
    si = jnp.where((q & 2) == 2, -si, si)
    return co, si


def halves(x):
    hi = x.astype(BF16)
    return hi, (x - hi.astype(F32)).astype(BF16)


def mm(a, b):
    return jnp.dot(a, b, preferred_element_type=F32)


def row_chunks():
    return [pl.ds(r, CHUNK) for r in range(0, PATCH, CHUNK)]


def fused_kernel(
    volume_in, paths_in, steps_in, probe_in, measured_in, jitter_in, tables_in,
    out, total,
    volume, measured, tables, paths, steps, jitter, load_sems,
    xa, zv, xo, xi, zs, zr, phase, cosf, sinf, acc, back, pair_g, ga, probe2, wave, xs, vs, err, mbuf,
    send_sems, recv_sems,
):
    g = lax.axis_index("blk")
    w = lax.axis_index("wide")
    x, zh = g // 2, g % 2
    zl, y, core = w // 16, (w // 2) % 8, w % 2
    z = zh * 4 + zl

    def device(x_, y_, z_, core_):
        return (x_ * 2 + z_ // 4, (z_ % 4) * 16 + y_ * 2 + core_)

    x_up, x_down, x_far = (x + 1) % 4, (x + 3) % 4, (x + 2) % 4
    ring = [(x_up * 2 + zh, w), (x_down * 2 + zh, w), (x_far * 2 + zh, w)]
    across = (g + 1 - 2 * zh, w)
    groups = (
        (y, [device(x, (y + k) % 8, z, core) for k in range(1, 8)]),
        (z, [device(x, y, (z + k) % 8, core) for k in range(1, 8)]),
        (x * 2 + core, [device((x + k // 2) % 4, y, z, (core + k) % 2) for k in range(1, 8)]),
    )
    near = [(-1, w >= 1), (1, w < N_WIDE - 1), (-2, w >= 2), (2, w < N_WIDE - 2)]

    counter = [0]
    pending = []

    class Group:
        def __init__(self, moves, totals):
            k = counter[0]
            counter[0] += 1

            def describe(src, dst, device_id):
                return pltpu.make_async_remote_copy(
                    src_ref=src, dst_ref=dst, send_sem=send_sems.at[k], recv_sem=recv_sems.at[k],
                    device_id=device_id, device_id_type=MESH,
                )

            self.moves = [describe(*m) for m in moves]
            self.totals = [(describe(ref, ref, ring[0]), cond) for ref, cond in totals]

        def start(self, which=None, conds=None):
            for k in range(len(self.moves)) if which is None else which:
                guarded(conds[k] if conds else None, self.moves[k].start)
            if self not in pending:
                pending.append(self)

        def arrive(self):
            for c, cond in self.totals:
                guarded(cond, c.wait_recv)

        def sent(self):
            for c, cond in self.totals:
                guarded(cond, c.wait_send)

    def guarded(cond, f):
        if cond is None:
            f()
        else:
            pl.when(cond)(f)

    near_conds = [cond for _, cond in near]
    at_end = (w == 0) | (w == N_WIDE - 1)
    by_end = (w == 1) | (w == N_WIDE - 2)
    inner = (w > 1) & (w < N_WIDE - 2)

    def near_group(moves, c):
        return Group(moves, [(back.at[c, pl.ds(0, n)], cond) for n, cond in ((112, inner), (88, by_end), (56, at_end))])

    tile = [slice(c * 128, c * 128 + 128) for c in range(TILES)]
    hop = {
        c: Group([(volume.at[:, :, tile[c]], xa.at[k, c], ring[k]) for k in range(3)], [(xa.at[:, c], None)])
        for c in range(TILES) if c not in Z_FIRST
    }
    raw = {c: Group([(volume.at[:, :, tile[c]], zv.at[c], across)], [(zv.at[c], None)]) for c in Z_FIRST}
    spread = {c: Group([(xo.at[c, k], xi.at[c, k], ring[k]) for k in range(3)], [(xi.at[c], None)]) for c in Z_FIRST}
    cross = {c: Group([(zs.at[c], zr.at[c], across)], [(zr.at[c], None)]) for c in range(TILES) if c not in Z_FIRST}
    rows_sent = {-1: (56, 32, 88), 1: (56, 32, 24), -2: (56, 24, 120), 2: (64, 24, 0)}
    halo = [
        near_group([(phase.at[c, pl.ds(rows_sent[d][0], rows_sent[d][1]), :], phase.at[c, pl.ds(rows_sent[d][2], rows_sent[d][1]), :],
                     (g, jnp.clip(w + d, 0, N_WIDE - 1))) for d, _ in near], c)
        for c in range(TILES)
    ]
    rows_back = {-1: (24, 32, 0), 1: (88, 32, 32), -2: (0, 24, 64), 2: (120, 24, 88)}
    ret = [
        near_group([(acc.at[c + 1, pl.ds(rows_back[d][0], rows_back[d][1]), :], back.at[c, pl.ds(rows_back[d][2], rows_back[d][1]), :],
                     (g, jnp.clip(w + d, 0, N_WIDE - 1))) for d, _ in near], c)
        for c in range(TILES)
    ]
    gcross = [Group([(pair_g.at[c, 0], pair_g.at[c, 1], across)], [(zr.at[c], None)]) for c in range(TILES)]
    ghop = [
        Group([(pair_g.at[c, h], ga.at[k, c, h], ring[k]) for h in range(2) for k in range(3)], [(ga.at[:, c], None)])
        for c in range(TILES)
    ]
    sums = [Group([(mbuf.at[s, groups[s][0]], mbuf.at[s, groups[s][0]], p) for p in groups[s][1]], [(mbuf.at[s, pl.ds(0, 7)], None)]) for s in range(3)]

    loads = [
        pltpu.make_async_copy(src, dst, load_sems.at[k])
        for k, (src, dst) in enumerate((
            (volume_in, volume), (probe_in, probe2.at[:, pl.ds(0, PATCH)]), (probe_in, probe2.at[:, pl.ds(PATCH, PATCH)]),
            (paths_in, paths), (steps_in, steps), (jitter_in, jitter), (measured_in, measured), (tables_in, tables),
        ))
    ]
    barrier = pltpu.get_barrier_semaphore()
    for _, members in groups:
        for p in members:
            pl.semaphore_signal(barrier, inc=1, device_id=p, device_id_type=MESH)
    for d, cond in near:
        @pl.when(cond)
        def _():
            pl.semaphore_signal(barrier, inc=1, device_id=(g, jnp.clip(w + d, 0, N_WIDE - 1)), device_id_type=MESH)

    for c in loads:
        c.start()
    for t in (0, TILES + 1):
        cosf[t] = jnp.zeros((FRAME, 128), F32)
        sinf[t] = jnp.zeros((FRAME, 128), F32)
    acc[...] = jnp.zeros(acc.shape, F32)
    err[...] = jnp.zeros(err.shape, F32)

    neighbours = sum(cond.astype(jnp.int32) for _, cond in near)
    loads[0].wait()
    with jax.named_scope("wait"):
        pl.semaphore_wait(barrier, 21 + neighbours)
    for c in Z_FIRST:
        raw[c].start()
    for c in hop:
        hop[c].start()
    for c in loads[1:]:
        c.wait()

    slabs = [g, x_down * 2 + zh, x_up * 2 + zh, x_far * 2 + zh]

    partner = g + 1 - 2 * zh

    def stage_b_across(c):
        raw[c].arrive()

        def both(angle):
            s = jnp.zeros((ROWS, 128), F32)
            for l in range(2):
                s = s + paths[angle, l, g] * volume[l, :, tile[c]] + paths[angle, l, partner] * zv[c, l]
            return s

        for k, x_ in enumerate((x_up, x_down, x_far)):
            xo[c, k] = both(x_ * 2 + zh)
            spread[c].start([k])
        phase[c, TOP : TOP + ROWS, :] = both(g)

    def stage_b(c):
        if c in Z_FIRST:
            return stage_b_across(c)
        hop[c].arrive()
        blocks = [(volume[l, :, tile[c]], xa[0, c, l], xa[1, c, l], xa[2, c, l]) for l in range(2)]

        def term(angle):
            s = jnp.zeros((ROWS, 128), F32)
            for l in range(2):
                for k in range(4):
                    s = s + paths[angle, l, slabs[k]] * blocks[l][k]
            return s

        zs[c] = term(g + 1 - 2 * zh)
        cross[c].start()
        phase[c, TOP : TOP + ROWS, :] = term(g)

    def stage_c(c):
        if c in Z_FIRST:
            spread[c].arrive()
            rest = xi[c, 0] + xi[c, 1] + xi[c, 2]
        else:
            cross[c].arrive()
            rest = zr[c]
        phase[c, TOP : TOP + ROWS, :] = phase[c, TOP : TOP + ROWS, :] + rest
        halo[c].start(conds=near_conds)

    first = TOP - ROWS * w

    def stage_d(c):
        halo[c].arrive()
        for r in range(0, FRAME, 24):
            row = lax.broadcasted_iota(jnp.int32, (24, 128), 0) + r
            inside = (row >= first) & (row < first + ROWS * N_WIDE)
            co, si = cos_sin(jnp.where(inside, phase[c, r : r + 24, :], 0.0))
            cosf[c + 1, r : r + 24, :] = jnp.where(inside, co, 0.0)
            sinf[c + 1, r : r + 24, :] = jnp.where(inside, si, 0.0)

    def masks(pair, p):
        j = 2 * pair + p
        jr = jitter[0, j]
        s = (24 if p else 88) + jitter[1, j]
        lane = lax.broadcasted_iota(jnp.int32, (CHUNK, PATCH), 1) >= s
        row = lax.broadcasted_iota(jnp.int32, (16, PATCH), 0) >= jr
        return j, jr, s, lane, row

    def put_rows(slot, p, c, a, b):
        at = slice(p * PATCH + c, p * PATCH + c + CHUNK)
        for k, x in enumerate((a, b)):
            hi, lo = halves(x)
            xs[slot, at, k * 128 : k * 128 + 128] = hi
            xs[slot, at, 256 + k * 128 : 256 + k * 128 + 128] = lo

    def right(slot, th, tl):
        x = xs[slot]
        return mm(jnp.concatenate([x, x[:, :256]], 1), jnp.concatenate([th, th, tl], 0))

    def to_cols(slot, u):
        for p in range(2):
            for k in range(2):
                for c in range(0, PATCH, CHUNK):
                    hi, lo = halves(u[p * PATCH + c : p * PATCH + c + CHUNK, k * 128 : k * 128 + 128])
                    vs[slot, k * PATCH + c : k * PATCH + c + CHUNK, p * 128 : p * 128 + 128] = hi
                    vs[slot, 256 + k * PATCH + c : 256 + k * PATCH + c + CHUNK, p * 128 : p * 128 + 128] = lo

    def left(slot, th, tl):
        v = vs[slot]
        return mm(jnp.concatenate([th, th, tl], 1), jnp.concatenate([v, v[:256]], 0))

    def waves(pair, slot):
        for p in range(2):
            j, jr, s, lane, row = masks(pair, p)
            t = pair + p
            for c in range(0, PATCH, CHUNK):
                def pick(ref):
                    a = ref[t, c : c + CHUNK, :]
                    b = ref[t + 1, c : c + CHUNK, :]
                    if c == 0:
                        a0 = jnp.where(row, a[:16], ref[t, PATCH:, :])
                        b0 = jnp.where(row, b[:16], ref[t + 1, PATCH:, :])
                        a = jnp.concatenate([a0, a[16:]], 0)
                        b = jnp.concatenate([b0, b[16:]], 0)
                    return jnp.where(lane, a, b)
                o_r, o_i = pick(cosf), pick(sinf)
                at = pl.ds(PATCH - jr + c, CHUNK)
                p_r = pltpu.roll(probe2[0, at, :], s, 1)
                p_i = pltpu.roll(probe2[1, at, :], s, 1)
                w_r = p_r * o_r - p_i * o_i
                w_i = p_r * o_i + p_i * o_r
                wave[slot, p, 0, c : c + CHUNK, :] = w_r
                wave[slot, p, 1, c : c + CHUNK, :] = w_i
                put_rows(slot, p, c, w_r, w_i)
    def pointwise(pair, slot, y):
        e = err[...]
        for p in range(2):
            j = 2 * pair + p
            for c in range(0, PATCH, CHUNK):
                f_r = y[c : c + CHUNK, p * 128 : p * 128 + 128]
                f_i = y[PATCH + c : PATCH + c + CHUNK, p * 128 : p * 128 + 128]
                m2 = f_r * f_r + f_i * f_i
                target = measured[j, c : c + CHUNK, :].astype(F32)
                d = jnp.sqrt(m2) - target
                d2 = d * d
                for k in range(0, CHUNK, 8):
                    e = e + d2[k : k + 8]
                ratio = target * lax.rsqrt(jnp.maximum(m2, 0.0625))
                put_rows(2 + slot, p, c, ratio * f_r, ratio * f_i)
        err[...] = e
    def accumulate(pair, slot, y):
        for p in range(2):
            j, jr, s, lane, row = masks(pair, p)
            t = pair + p
            for c in range(0, PATCH, CHUNK):
                b_r = y[c : c + CHUNK, p * 128 : p * 128 + 128]
                b_i = y[PATCH + c : PATCH + c + CHUNK, p * 128 : p * 128 + 128]
                g = wave[slot, p, 0, c : c + CHUNK, :] * b_i - wave[slot, p, 1, c : c + CHUNK, :] * b_r
                for tile, part in ((t, jnp.where(lane, g, 0.0)), (t + 1, jnp.where(lane, 0.0, g))):
                    if c == 0:
                        acc[tile, PATCH:, :] += jnp.where(row, 0.0, part[:16])
                        part = jnp.concatenate([jnp.where(row, part[:16], 0.0), part[16:]], 0)
                    acc[tile, c : c + CHUNK, :] += part

    def stage_e(i):
        t1h, t1l, t2h, t2l = (tables[k] for k in range(4))
        ahead, behind = i < PCOLS // 2, i > 0
        if behind:
            u2 = right(2 + (i - 1) % 2, t2h, t2l)
        if ahead:
            waves(i, i % 2)
            u1 = right(i % 2, t1h, t1l)
        if behind:
            to_cols(1, u2)
            y2 = left(1, t1h, t1l)
        if ahead:
            to_cols(0, u1)
            y1 = left(0, t2h, t2l)
        if behind:
            accumulate(i - 1, (i - 1) % 2, y2)
        if ahead:
            pointwise(i, i % 2, y1)

    def stage_f(c):
        ret[c].start(conds=near_conds)

    def stage_g(c):
        pair_g[c, 0] = acc[c + 1, TOP : TOP + ROWS, :]
        ret[c].arrive()
        for k, (d, cond) in enumerate(near):
            ok = {1: w >= 1, -1: w < N_WIDE - 1, 2: w >= 2, -2: w < N_WIDE - 2}[d]
            lo, n, at = {-1: (0, 32, 0), 1: (0, 32, 32), -2: (8, 24, 64), 2: (0, 24, 88)}[d]

            @pl.when(ok)
            def _():
                pair_g[c, 0, lo : lo + n, :] = pair_g[c, 0, lo : lo + n, :] + back[c, at : at + n, :]

        gcross[c].start()
        ghop[c].start((0, 1, 2))

    def stage_h(c):
        gcross[c].arrive()
        ghop[c].start((3, 4, 5))

    angles = [g, g + 1 - 2 * zh, x_down * 2 + zh, x_down * 2 + 1 - zh, x_up * 2 + zh, x_up * 2 + 1 - zh, x_far * 2 + zh, x_far * 2 + 1 - zh]

    def stage_j(c):
        ghop[c].arrive()
        grads = [pair_g[c, 0], pair_g[c, 1], *(ga[k, c, h] for k in range(3) for h in range(2))]
        for l in range(2):
            s = jnp.zeros((ROWS, 128), F32)
            for a, gr in zip(angles, grads):
                s = s + (steps[a] * paths[a, l, g]) * gr
            out[l, :, tile[c]] = s

    def misfit_send(s, value):
        mbuf[s, pl.ds(groups[s][0], 1)] = value[None]
        sums[s].start()

    def misfit_take(s):
        sums[s].arrive()
        v = mbuf[s, 0]
        for k in range(1, 8):
            v = v + mbuf[s, k]
        return v

    def stage_m(c):
        value = misfit_take(c - 1) if c else err[...]
        if c < 3:
            misfit_send(c, value)
        else:
            total[0] = jnp.sum(value)

    stages = dict(zip("BCDEFGHJM", (stage_b, stage_c, stage_d, stage_e, stage_f, stage_g, stage_h, stage_j, stage_m)))
    def drop(count):
        for c in pending[:count]:
            c.sent()
        del pending[:count]

    plan = order()
    tail = plan.index(("F", TILES - 1)) + 1
    for at, (name, c) in enumerate(plan):
        if at >= tail and len(pending) > 9:
            drop(3)
        with jax.named_scope(f"{name}{c}"):
            stages[name](c)
    with jax.named_scope("end"):
        drop(len(pending))


STEP = 1.0
Z_FIRST = (1, 2)


def order():
    tiles = range(TILES)
    due, ready, turn = [], [], {True: 0, False: 0}
    for c in tiles:
        z_first = c in Z_FIRST
        k = turn[z_first]
        turn[z_first] += 1
        begin = 6.9 + 1.4 * k if z_first else 2.2 + 1.4 * k
        joined = begin + (2.7 if z_first else 6.6)
        due += [(begin, "B", c), (joined, "C", c), (joined + 3.7, "D", c)]
        ready.append(joined + 3.7)
    done, now = [], 0.0
    for i in range(TILES + 1):
        now = max(now, max(ready[: i + 2]) + 0.01)
        due.append((now, "E", i))
        now += STEP
        done.append(now - 0.01)
    for c in tiles:
        t = done[min(c + 2, TILES)]
        due += [(t, "F", c), (t + 3.8 - 0.15 * c, "G", c), (t + 9.3 - 0.15 * c, "H", c), (t + 13.5 - 0.15 * c, "J", c)]
    due += [(done[TILES - 1] - 0.001 + t, "M", c) for c, t in enumerate((0.0, 4.6, 10.4, 15.0))]
    return [(name, c) for _, name, c in sorted(due)]


def fused(volume, paths, steps, probe, measured, jitter):
    vm = pl.BlockSpec(memory_space=pltpu.VMEM)
    hbm = pl.BlockSpec(memory_space=pl.ANY)
    sm = pl.BlockSpec(memory_space=pltpu.SMEM)
    copies = TILES * 6 + 3
    grid = pltpu.VMEM((TILES + 2, FRAME, 128), F32)
    return pl.pallas_call(
        fused_kernel,
        out_shape=(pltpu.VMEM((2, ROWS, COLS), F32), jax.ShapeDtypeStruct((1,), F32)),
        in_specs=[hbm] * 7,
        out_specs=(vm, sm),
        scratch_shapes=[
            pltpu.VMEM((2, ROWS, COLS), F32),
            pltpu.VMEM((PCOLS, PATCH, PATCH), BF16),
            pltpu.VMEM((4, 2 * PATCH, 2 * PATCH), BF16),
            pltpu.SMEM((8, 2, 8), F32),
            pltpu.SMEM((8,), F32),
            pltpu.SMEM((2, PCOLS), jnp.int32),
            pltpu.SemaphoreType.DMA((8,)),
            pltpu.VMEM((3, TILES, 2, ROWS, 128), F32),
            pltpu.VMEM((TILES, 2, ROWS, 128), F32),
            pltpu.VMEM((TILES, 3, ROWS, 128), F32),
            pltpu.VMEM((TILES, 3, ROWS, 128), F32),
            pltpu.VMEM((TILES, ROWS, 128), F32),
            pltpu.VMEM((TILES, ROWS, 128), F32),
            pltpu.VMEM((TILES, FRAME, 128), F32),
            grid, grid, grid,
            pltpu.VMEM((TILES, 112, 128), F32),
            pltpu.VMEM((TILES, 2, ROWS, 128), F32),
            pltpu.VMEM((3, TILES, 2, ROWS, 128), F32),
            pltpu.VMEM((2, 2 * PATCH, PATCH), F32),
            pltpu.VMEM((2, 2, 2, PATCH, PATCH), F32),
            pltpu.VMEM((4, 2 * PATCH, 512), BF16),
            pltpu.VMEM((2, 512, 2 * PATCH), BF16),
            pltpu.VMEM((8, 128), F32),
            pltpu.VMEM((3, 8, 8, 128), F32),
            pltpu.SemaphoreType.DMA((copies,)),
            pltpu.SemaphoreType.DMA((copies,)),
        ],
        compiler_params=pltpu.CompilerParams(collective_id=0, has_side_effects=True),
        name="fused",
    )(volume, paths, steps, probe, measured, jitter, jnp.asarray(dft_tables()))


def body(volume, path_lengths, probe, measured, jitter, step_sizes):
    paths = jnp.transpose(path_lengths, (0, 2, 1))
    update, total = fused(volume[0], paths, step_sizes, probe, measured[0, 0], jitter[:, 0, 0])
    return volume - update[None], total[0]


def solution(mesh):
    in_specs = (
        P("blk", None, "wide", None),
        P(),
        P(),
        P("blk", "wide", None, None, None),
        P(None, "blk", "wide", None),
        P(),
    )
    out_specs = (P("blk", None, "wide", None), P())
    return jax.shard_map(body, mesh=mesh, in_specs=in_specs, out_specs=out_specs, check_vma=False)
```

```python
import functools

import jax
import jax.numpy as jnp
import ml_dtypes
import numpy as np
from jax import lax
from jax.experimental import pallas as pl
from jax.experimental.pallas import tpu as pltpu
from jax.sharding import PartitionSpec as P

ROWS = 32
COLS = 896
PATCH = 128
PCOLS = 14
N_BLK = 8
N_WIDE = 64
MESH = pl.DeviceIdType.MESH
TILES = COLS // 128
FRAME = 144
TOP = 56
CHUNK = 32
F32 = jnp.float32
BF16 = jnp.bfloat16


def dft_tables():
    n = np.arange(PATCH)
    angle = (n[:, None] * n[None, :] % PATCH) * (2 * np.pi / PATCH)
    c = np.cos(angle) / np.sqrt(float(PATCH))
    s = -np.sin(angle) / np.sqrt(float(PATCH))
    out = []
    for t in (np.block([[c, s], [-s, c]]), np.block([[c, -s], [s, c]])):
        t = t.astype(np.float32)
        hi = t.astype(ml_dtypes.bfloat16)
        out += [hi, (t - hi.astype(np.float32)).astype(ml_dtypes.bfloat16)]
    return np.stack(out)


def cos_sin(x):
    k = jnp.floor(x * np.float32(2 / np.pi) + np.float32(0.5))
    r = x - k * np.float32(1.5703125)
    r = r - k * np.float32(4.837512969970703125e-4)
    r = r - k * np.float32(7.54978995489188216e-8)
    z = r * r
    sn = ((np.float32(-1.9515295891e-4) * z + np.float32(8.3321608736e-3)) * z - np.float32(1.6666654611e-1)) * z * r + r
    cs = ((np.float32(2.443315711809948e-5) * z - np.float32(1.388731625493765e-3)) * z + np.float32(4.166664568298827e-2)) * z * z
    cs = cs - np.float32(0.5) * z + np.float32(1.0)
    q = k.astype(jnp.int32)
    swap = (q & 1) == 1
    co = jnp.where(swap, sn, cs)
    si = jnp.where(swap, cs, sn)
    co = jnp.where(((q + 1) & 2) == 2, -co, co)
    si = jnp.where((q & 2) == 2, -si, si)
    return co, si


def halves(x):
    hi = x.astype(BF16)
    return hi, (x - hi.astype(F32)).astype(BF16)


def mm(a, b):
    return jnp.dot(a, b, preferred_element_type=F32)


def row_chunks():
    return [pl.ds(r, CHUNK) for r in range(0, PATCH, CHUNK)]


def fused_kernel(
    volume_in, paths_in, steps_in, probe_in, measured_in, jitter_in, tables_in,
    out, total,
    volume, measured, tables, paths, steps, jitter, load_sems,
    xa, zv, xo, xi, zs, zr, phase, cosf, sinf, acc, back, pair_g, ga, probe2, wave, xs, vs, err, mbuf,
    send_sems, recv_sems,
):
    g = lax.axis_index("blk")
    w = lax.axis_index("wide")
    x, zh = g // 2, g % 2
    zl, y, core = w // 16, (w // 2) % 8, w % 2
    z = zh * 4 + zl

    def device(x_, y_, z_, core_):
        return (x_ * 2 + z_ // 4, (z_ % 4) * 16 + y_ * 2 + core_)

    x_up, x_down, x_far = (x + 1) % 4, (x + 3) % 4, (x + 2) % 4
    ring = [(x_up * 2 + zh, w), (x_down * 2 + zh, w), (x_far * 2 + zh, w)]
    across = (g + 1 - 2 * zh, w)
    groups = (
        (y, [device(x, (y + k) % 8, z, core) for k in range(1, 8)]),
        (z, [device(x, y, (z + k) % 8, core) for k in range(1, 8)]),
        (x * 2 + core, [device((x + k // 2) % 4, y, z, (core + k) % 2) for k in range(1, 8)]),
    )
    near = [(-1, w >= 1), (1, w < N_WIDE - 1), (-2, w >= 2), (2, w < N_WIDE - 2)]

    counter = [0]
    pending = []

    class Group:
        def __init__(self, moves, totals):
            k = counter[0]
            counter[0] += 1

            def describe(src, dst, device_id):
                return pltpu.make_async_remote_copy(
                    src_ref=src, dst_ref=dst, send_sem=send_sems.at[k], recv_sem=recv_sems.at[k],
                    device_id=device_id, device_id_type=MESH,
                )

            self.moves = [describe(*m) for m in moves]
            self.totals = [(describe(ref, ref, ring[0]), cond) for ref, cond in totals]

        def start(self, which=None, conds=None):
            for k in range(len(self.moves)) if which is None else which:
                guarded(conds[k] if conds else None, self.moves[k].start)
            if self not in pending:
                pending.append(self)

        def arrive(self):
            for c, cond in self.totals:
                guarded(cond, c.wait_recv)

        def sent(self):
            for c, cond in self.totals:
                guarded(cond, c.wait_send)

    def guarded(cond, f):
        if cond is None:
            f()
        else:
            pl.when(cond)(f)

    near_conds = [cond for _, cond in near]
    at_end = (w == 0) | (w == N_WIDE - 1)
    by_end = (w == 1) | (w == N_WIDE - 2)
    inner = (w > 1) & (w < N_WIDE - 2)

    def near_group(moves, c):
        return Group(moves, [(back.at[c, pl.ds(0, n)], cond) for n, cond in ((112, inner), (88, by_end), (56, at_end))])

    tile = [slice(c * 128, c * 128 + 128) for c in range(TILES)]
    hop = {
        c: Group([(volume.at[:, :, tile[c]], xa.at[k, c], ring[k]) for k in range(3)], [(xa.at[:, c], None)])
        for c in range(TILES) if c not in Z_FIRST
    }
    raw = {c: Group([(volume.at[:, :, tile[c]], zv.at[c], across)], [(zv.at[c], None)]) for c in Z_FIRST}
    spread = {c: Group([(xo.at[c, k], xi.at[c, k], ring[k]) for k in range(3)], [(xi.at[c], None)]) for c in Z_FIRST}
    cross = {c: Group([(zs.at[c], zr.at[c], across)], [(zr.at[c], None)]) for c in range(TILES) if c not in Z_FIRST}
    rows_sent = {-1: (56, 32, 88), 1: (56, 32, 24), -2: (56, 24, 120), 2: (64, 24, 0)}
    halo = [
        near_group([(phase.at[c, pl.ds(rows_sent[d][0], rows_sent[d][1]), :], phase.at[c, pl.ds(rows_sent[d][2], rows_sent[d][1]), :],
                     (g, jnp.clip(w + d, 0, N_WIDE - 1))) for d, _ in near], c)
        for c in range(TILES)
    ]
    rows_back = {-1: (24, 32, 0), 1: (88, 32, 32), -2: (0, 24, 64), 2: (120, 24, 88)}
    ret = [
        near_group([(acc.at[c + 1, pl.ds(rows_back[d][0], rows_back[d][1]), :], back.at[c, pl.ds(rows_back[d][2], rows_back[d][1]), :],
                     (g, jnp.clip(w + d, 0, N_WIDE - 1))) for d, _ in near], c)
        for c in range(TILES)
    ]
    gcross = [Group([(pair_g.at[c, 0], pair_g.at[c, 1], across)], [(zr.at[c], None)]) for c in range(TILES)]
    ghop = [
        Group([(pair_g.at[c, h], ga.at[k, c, h], ring[k]) for h in range(2) for k in range(3)], [(ga.at[:, c], None)])
        for c in range(TILES)
    ]
    sums = [Group([(mbuf.at[s, groups[s][0]], mbuf.at[s, groups[s][0]], p) for p in groups[s][1]], [(mbuf.at[s, pl.ds(0, 7)], None)]) for s in range(3)]

    loads = [
        pltpu.make_async_copy(src, dst, load_sems.at[k])
        for k, (src, dst) in enumerate((
            (volume_in, volume), (probe_in, probe2.at[:, pl.ds(0, PATCH)]), (probe_in, probe2.at[:, pl.ds(PATCH, PATCH)]),
            (paths_in, paths), (steps_in, steps), (jitter_in, jitter), (measured_in, measured), (tables_in, tables),
        ))
    ]
    barrier = pltpu.get_barrier_semaphore()
    for _, members in groups:
        for p in members:
            pl.semaphore_signal(barrier, inc=1, device_id=p, device_id_type=MESH)
    for d, cond in near:
        @pl.when(cond)
        def _():
            pl.semaphore_signal(barrier, inc=1, device_id=(g, jnp.clip(w + d, 0, N_WIDE - 1)), device_id_type=MESH)

    for c in loads:
        c.start()
    for t in (0, TILES + 1):
        cosf[t] = jnp.zeros((FRAME, 128), F32)
        sinf[t] = jnp.zeros((FRAME, 128), F32)
    acc[...] = jnp.zeros(acc.shape, F32)
    err[...] = jnp.zeros(err.shape, F32)

    neighbours = sum(cond.astype(jnp.int32) for _, cond in near)
    loads[0].wait()
    with jax.named_scope("wait"):
        pl.semaphore_wait(barrier, 21 + neighbours)
    for c in Z_FIRST:
        raw[c].start()
    for c in hop:
        hop[c].start()
    for c in loads[1:]:
        c.wait()

    slabs = [g, x_down * 2 + zh, x_up * 2 + zh, x_far * 2 + zh]

    partner = g + 1 - 2 * zh

    def stage_b_across(c):
        raw[c].arrive()

        def both(angle):
            s = jnp.zeros((ROWS, 128), F32)
            for l in range(2):
                s = s + paths[angle, l, g] * volume[l, :, tile[c]] + paths[angle, l, partner] * zv[c, l]
            return s

        for k, x_ in enumerate((x_up, x_down, x_far)):
            xo[c, k] = both(x_ * 2 + zh)
            spread[c].start([k])
        phase[c, TOP : TOP + ROWS, :] = both(g)

    def stage_b(c):
        if c in Z_FIRST:
            return stage_b_across(c)
        hop[c].arrive()
        blocks = [(volume[l, :, tile[c]], xa[0, c, l], xa[1, c, l], xa[2, c, l]) for l in range(2)]

        def term(angle):
            s = jnp.zeros((ROWS, 128), F32)
            for l in range(2):
                for k in range(4):
                    s = s + paths[angle, l, slabs[k]] * blocks[l][k]
            return s

        zs[c] = term(g + 1 - 2 * zh)
        cross[c].start()
        phase[c, TOP : TOP + ROWS, :] = term(g)

    def stage_c(c):
        if c in Z_FIRST:
            spread[c].arrive()
            rest = xi[c, 0] + xi[c, 1] + xi[c, 2]
        else:
            cross[c].arrive()
            rest = zr[c]
        phase[c, TOP : TOP + ROWS, :] = phase[c, TOP : TOP + ROWS, :] + rest
        halo[c].start(conds=near_conds)

    first = TOP - ROWS * w

    def stage_d(c):
        halo[c].arrive()
        for r in range(0, FRAME, 24):
            row = lax.broadcasted_iota(jnp.int32, (24, 128), 0) + r
            inside = (row >= first) & (row < first + ROWS * N_WIDE)
            co, si = cos_sin(jnp.where(inside, phase[c, r : r + 24, :], 0.0))
            cosf[c + 1, r : r + 24, :] = jnp.where(inside, co, 0.0)
            sinf[c + 1, r : r + 24, :] = jnp.where(inside, si, 0.0)

    def masks(pair, p):
        j = 2 * pair + p
        jr = jitter[0, j]
        s = (24 if p else 88) + jitter[1, j]
        lane = lax.broadcasted_iota(jnp.int32, (CHUNK, PATCH), 1) >= s
        row = lax.broadcasted_iota(jnp.int32, (16, PATCH), 0) >= jr
        return j, jr, s, lane, row

    def put_rows(slot, p, c, a, b):
        at = slice(p * PATCH + c, p * PATCH + c + CHUNK)
        for k, x in enumerate((a, b)):
            hi, lo = halves(x)
            xs[slot, at, k * 128 : k * 128 + 128] = hi
            xs[slot, at, 256 + k * 128 : 256 + k * 128 + 128] = lo

    def right(slot, th, tl):
        x = xs[slot]
        return mm(jnp.concatenate([x, x[:, :256]], 1), jnp.concatenate([th, th, tl], 0))

    def to_cols(slot, u):
        for p in range(2):
            for k in range(2):
                for c in range(0, PATCH, CHUNK):
                    hi, lo = halves(u[p * PATCH + c : p * PATCH + c + CHUNK, k * 128 : k * 128 + 128])
                    vs[slot, k * PATCH + c : k * PATCH + c + CHUNK, p * 128 : p * 128 + 128] = hi
                    vs[slot, 256 + k * PATCH + c : 256 + k * PATCH + c + CHUNK, p * 128 : p * 128 + 128] = lo

    def left(slot, th, tl):
        v = vs[slot]
        return mm(jnp.concatenate([th, th, tl], 1), jnp.concatenate([v, v[:256]], 0))

    def waves(pair, slot):
        for p in range(2):
            j, jr, s, lane, row = masks(pair, p)
            t = pair + p
            for c in range(0, PATCH, CHUNK):
                def pick(ref):
                    a = ref[t, c : c + CHUNK, :]
                    b = ref[t + 1, c : c + CHUNK, :]
                    if c == 0:
                        a0 = jnp.where(row, a[:16], ref[t, PATCH:, :])
                        b0 = jnp.where(row, b[:16], ref[t + 1, PATCH:, :])
                        a = jnp.concatenate([a0, a[16:]], 0)
                        b = jnp.concatenate([b0, b[16:]], 0)
                    return jnp.where(lane, a, b)
                o_r, o_i = pick(cosf), pick(sinf)
                at = pl.ds(PATCH - jr + c, CHUNK)
                p_r = pltpu.roll(probe2[0, at, :], s, 1)
                p_i = pltpu.roll(probe2[1, at, :], s, 1)
                w_r = p_r * o_r - p_i * o_i
                w_i = p_r * o_i + p_i * o_r
                wave[slot, p, 0, c : c + CHUNK, :] = w_r
                wave[slot, p, 1, c : c + CHUNK, :] = w_i
                put_rows(slot, p, c, w_r, w_i)
    def pointwise(pair, slot, y):
        e = err[...]
        for p in range(2):
            j = 2 * pair + p
            for c in range(0, PATCH, CHUNK):
                f_r = y[c : c + CHUNK, p * 128 : p * 128 + 128]
                f_i = y[PATCH + c : PATCH + c + CHUNK, p * 128 : p * 128 + 128]
                m2 = f_r * f_r + f_i * f_i
                target = measured[j, c : c + CHUNK, :].astype(F32)
                d = jnp.sqrt(m2) - target
                d2 = d * d
                for k in range(0, CHUNK, 8):
                    e = e + d2[k : k + 8]
                ratio = target * lax.rsqrt(jnp.maximum(m2, 0.0625))
                put_rows(2 + slot, p, c, ratio * f_r, ratio * f_i)
        err[...] = e
    def accumulate(pair, slot, y):
        for p in range(2):
            j, jr, s, lane, row = masks(pair, p)
            t = pair + p
            for c in range(0, PATCH, CHUNK):
                b_r = y[c : c + CHUNK, p * 128 : p * 128 + 128]
                b_i = y[PATCH + c : PATCH + c + CHUNK, p * 128 : p * 128 + 128]
                g = wave[slot, p, 0, c : c + CHUNK, :] * b_i - wave[slot, p, 1, c : c + CHUNK, :] * b_r
                for tile, part in ((t, jnp.where(lane, g, 0.0)), (t + 1, jnp.where(lane, 0.0, g))):
                    if c == 0:
                        acc[tile, PATCH:, :] += jnp.where(row, 0.0, part[:16])
                        part = jnp.concatenate([jnp.where(row, part[:16], 0.0), part[16:]], 0)
                    acc[tile, c : c + CHUNK, :] += part

    def stage_e(i):
        t1h, t1l, t2h, t2l = (tables[k] for k in range(4))
        ahead, behind = i < PCOLS // 2, i > 0
        if behind:
            u2 = right(2 + (i - 1) % 2, t2h, t2l)
        if ahead:
            waves(i, i % 2)
            u1 = right(i % 2, t1h, t1l)
        if behind:
            to_cols(1, u2)
            y2 = left(1, t1h, t1l)
        if ahead:
            to_cols(0, u1)
            y1 = left(0, t2h, t2l)
        if behind:
            accumulate(i - 1, (i - 1) % 2, y2)
        if ahead:
            pointwise(i, i % 2, y1)

    def stage_f(c):
        ret[c].start(conds=near_conds)

    def stage_g(c):
        pair_g[c, 0] = acc[c + 1, TOP : TOP + ROWS, :]
        ret[c].arrive()
        for k, (d, cond) in enumerate(near):
            ok = {1: w >= 1, -1: w < N_WIDE - 1, 2: w >= 2, -2: w < N_WIDE - 2}[d]
            lo, n, at = {-1: (0, 32, 0), 1: (0, 32, 32), -2: (8, 24, 64), 2: (0, 24, 88)}[d]

            @pl.when(ok)
            def _():
                pair_g[c, 0, lo : lo + n, :] = pair_g[c, 0, lo : lo + n, :] + back[c, at : at + n, :]

        gcross[c].start()
        ghop[c].start((0, 1, 2))

    def stage_h(c):
        gcross[c].arrive()
        ghop[c].start((3, 4, 5))

    angles = [g, g + 1 - 2 * zh, x_down * 2 + zh, x_down * 2 + 1 - zh, x_up * 2 + zh, x_up * 2 + 1 - zh, x_far * 2 + zh, x_far * 2 + 1 - zh]

    def stage_j(c):
        ghop[c].arrive()
        grads = [pair_g[c, 0], pair_g[c, 1], *(ga[k, c, h] for k in range(3) for h in range(2))]
        for l in range(2):
            s = jnp.zeros((ROWS, 128), F32)
            for a, gr in zip(angles, grads):
                s = s + (steps[a] * paths[a, l, g]) * gr
            out[l, :, tile[c]] = s

    def misfit_send(s, value):
        mbuf[s, pl.ds(groups[s][0], 1)] = value[None]
        sums[s].start()

    def misfit_take(s):
        sums[s].arrive()
        v = mbuf[s, 0]
        for k in range(1, 8):
            v = v + mbuf[s, k]
        return v

    def stage_m(c):
        value = misfit_take(c - 1) if c else err[...]
        if c < 3:
            misfit_send(c, value)
        else:
            total[...] = jnp.full((8, 128), jnp.sum(value), F32)

    stages = dict(zip("BCDEFGHJM", (stage_b, stage_c, stage_d, stage_e, stage_f, stage_g, stage_h, stage_j, stage_m)))
    def drop(count):
        for c in pending[:count]:
            c.sent()
        del pending[:count]

    plan = order()
    tail = plan.index(("F", TILES - 1)) + 1
    for at, (name, c) in enumerate(plan):
        if at >= tail and len(pending) > 9:
            drop(3)
        with jax.named_scope(f"{name}{c}"):
            stages[name](c)
    with jax.named_scope("end"):
        drop(len(pending))


STEP = 1.0
Z_FIRST = (1, 2)


def order():
    tiles = range(TILES)
    due, ready, turn = [], [], {True: 0, False: 0}
    for c in tiles:
        z_first = c in Z_FIRST
        k = turn[z_first]
        turn[z_first] += 1
        begin = 6.9 + 1.4 * k if z_first else 2.2 + 1.4 * k
        joined = begin + (2.7 if z_first else 6.6)
        due += [(begin, "B", c), (joined, "C", c), (joined + 3.7, "D", c)]
        ready.append(joined + 3.7)
    done, now = [], 0.0
    for i in range(TILES + 1):
        now = max(now, max(ready[: i + 2]) + 0.01)
        due.append((now, "E", i))
        now += STEP
        done.append(now - 0.01)
    for c in tiles:
        t = done[min(c + 2, TILES)]
        due += [(t, "F", c), (t + 3.8 - 0.15 * c, "G", c), (t + 9.3 - 0.15 * c, "H", c), (t + 13.5 - 0.15 * c, "J", c)]
    due += [(done[TILES - 1] - 0.001 + t, "M", c) for c, t in enumerate((0.0, 4.6, 10.4, 15.0))]
    return [(name, c) for _, name, c in sorted(due)]


def fused(volume, paths, steps, probe, measured, jitter):
    vm = pl.BlockSpec(memory_space=pltpu.VMEM)
    hbm = pl.BlockSpec(memory_space=pl.ANY)
    copies = TILES * 6 + 3
    grid = pltpu.VMEM((TILES + 2, FRAME, 128), F32)
    return pl.pallas_call(
        fused_kernel,
        out_shape=(pltpu.VMEM((2, ROWS, COLS), F32), pltpu.VMEM((8, 128), F32)),
        in_specs=[hbm] * 7,
        out_specs=(vm, vm),
        scratch_shapes=[
            pltpu.VMEM((2, ROWS, COLS), F32),
            pltpu.VMEM((PCOLS, PATCH, PATCH), BF16),
            pltpu.VMEM((4, 2 * PATCH, 2 * PATCH), BF16),
            pltpu.SMEM((8, 2, 8), F32),
            pltpu.SMEM((8,), F32),
            pltpu.SMEM((2, PCOLS), jnp.int32),
            pltpu.SemaphoreType.DMA((8,)),
            pltpu.VMEM((3, TILES, 2, ROWS, 128), F32),
            pltpu.VMEM((TILES, 2, ROWS, 128), F32),
            pltpu.VMEM((TILES, 3, ROWS, 128), F32),
            pltpu.VMEM((TILES, 3, ROWS, 128), F32),
            pltpu.VMEM((TILES, ROWS, 128), F32),
            pltpu.VMEM((TILES, ROWS, 128), F32),
            pltpu.VMEM((TILES, FRAME, 128), F32),
            grid, grid, grid,
            pltpu.VMEM((TILES, 112, 128), F32),
            pltpu.VMEM((TILES, 2, ROWS, 128), F32),
            pltpu.VMEM((3, TILES, 2, ROWS, 128), F32),
            pltpu.VMEM((2, 2 * PATCH, PATCH), F32),
            pltpu.VMEM((2, 2, 2, PATCH, PATCH), F32),
            pltpu.VMEM((4, 2 * PATCH, 512), BF16),
            pltpu.VMEM((2, 512, 2 * PATCH), BF16),
            pltpu.VMEM((8, 128), F32),
            pltpu.VMEM((3, 8, 8, 128), F32),
            pltpu.SemaphoreType.DMA((copies,)),
            pltpu.SemaphoreType.DMA((copies,)),
        ],
        compiler_params=pltpu.CompilerParams(collective_id=0, has_side_effects=True),
        name="fused",
    )(volume, paths, steps, probe, measured, jitter, jnp.asarray(dft_tables()))


def body(volume, path_lengths, probe, measured, jitter, step_sizes):
    paths = jnp.transpose(path_lengths, (0, 2, 1))
    update, total = fused(volume[0], paths, step_sizes, probe, measured[0, 0], jitter[:, 0, 0])
    return volume - update[None], total[0, 0]


def solution(mesh):
    in_specs = (
        P("blk", None, "wide", None),
        P(),
        P(),
        P("blk", "wide", None, None, None),
        P(None, "blk", "wide", None),
        P(),
    )
    out_specs = (P("blk", None, "wide", None), P())
    return jax.shard_map(body, mesh=mesh, in_specs=in_specs, out_specs=out_specs, check_vma=False)
```

```python
import functools

import jax
import jax.numpy as jnp
import ml_dtypes
import numpy as np
from jax import lax
from jax.experimental import pallas as pl
from jax.experimental.pallas import tpu as pltpu
from jax.sharding import PartitionSpec as P

ROWS = 32
COLS = 896
PATCH = 128
PCOLS = 14
N_BLK = 8
N_WIDE = 64
MESH = pl.DeviceIdType.MESH
TILES = COLS // 128
FRAME = 144
TOP = 56
CHUNK = 32
F32 = jnp.float32
BF16 = jnp.bfloat16


def dft_tables():
    n = np.arange(PATCH)
    angle = (n[:, None] * n[None, :] % PATCH) * (2 * np.pi / PATCH)
    c = np.cos(angle) / np.sqrt(float(PATCH))
    s = -np.sin(angle) / np.sqrt(float(PATCH))
    out = []
    for t in (np.block([[c, s], [-s, c]]), np.block([[c, -s], [s, c]])):
        t = t.astype(np.float32)
        hi = t.astype(ml_dtypes.bfloat16)
        out += [hi, (t - hi.astype(np.float32)).astype(ml_dtypes.bfloat16)]
    return np.stack(out)


def cos_sin(x):
    k = jnp.floor(x * np.float32(2 / np.pi) + np.float32(0.5))
    r = x - k * np.float32(1.5703125)
    r = r - k * np.float32(4.837512969970703125e-4)
    r = r - k * np.float32(7.54978995489188216e-8)
    z = r * r
    sn = ((np.float32(-1.9515295891e-4) * z + np.float32(8.3321608736e-3)) * z - np.float32(1.6666654611e-1)) * z * r + r
    cs = ((np.float32(2.443315711809948e-5) * z - np.float32(1.388731625493765e-3)) * z + np.float32(4.166664568298827e-2)) * z * z
    cs = cs - np.float32(0.5) * z + np.float32(1.0)
    q = k.astype(jnp.int32)
    swap = (q & 1) == 1
    co = jnp.where(swap, sn, cs)
    si = jnp.where(swap, cs, sn)
    co = jnp.where(((q + 1) & 2) == 2, -co, co)
    si = jnp.where((q & 2) == 2, -si, si)
    return co, si


def halves(x):
    hi = x.astype(BF16)
    return hi, (x - hi.astype(F32)).astype(BF16)


def mm(a, b):
    return jnp.dot(a, b, preferred_element_type=F32)


def row_chunks():
    return [pl.ds(r, CHUNK) for r in range(0, PATCH, CHUNK)]


def fused_kernel(
    volume_in, paths_in, steps_in, probe_in, measured_in, jitter_in, tables_in,
    out, total,
    volume, measured, tables, paths, steps, jitter, load_sems,
    xa, zv, xo, xi, zs, zr, phase, cosf, sinf, acc, back, pair_g, ga, probe2, wave, xs, vs, err, mbuf,
    send_sems, recv_sems,
):
    g = lax.axis_index("blk")
    w = lax.axis_index("wide")
    x, zh = g // 2, g % 2
    zl, y, core = w // 16, (w // 2) % 8, w % 2
    z = zh * 4 + zl

    def device(x_, y_, z_, core_):
        return (x_ * 2 + z_ // 4, (z_ % 4) * 16 + y_ * 2 + core_)

    x_up, x_down, x_far = (x + 1) % 4, (x + 3) % 4, (x + 2) % 4
    ring = [(x_up * 2 + zh, w), (x_down * 2 + zh, w), (x_far * 2 + zh, w)]
    across = (g + 1 - 2 * zh, w)
    groups = (
        (y, [device(x, (y + k) % 8, z, core) for k in range(1, 8)]),
        (z, [device(x, y, (z + k) % 8, core) for k in range(1, 8)]),
        (x * 2 + core, [device((x + k // 2) % 4, y, z, (core + k) % 2) for k in range(1, 8)]),
    )
    near = [(-1, w >= 1), (1, w < N_WIDE - 1), (-2, w >= 2), (2, w < N_WIDE - 2)]

    counter = [0]
    pending = []

    class Group:
        def __init__(self, moves, totals):
            k = counter[0]
            counter[0] += 1

            def describe(src, dst, device_id):
                return pltpu.make_async_remote_copy(
                    src_ref=src, dst_ref=dst, send_sem=send_sems.at[k], recv_sem=recv_sems.at[k],
                    device_id=device_id, device_id_type=MESH,
                )

            self.moves = [describe(*m) for m in moves]
            self.totals = [(describe(ref, ref, ring[0]), cond) for ref, cond in totals]

        def start(self, which=None, conds=None):
            for k in range(len(self.moves)) if which is None else which:
                guarded(conds[k] if conds else None, self.moves[k].start)
            if self not in pending:
                pending.append(self)

        def arrive(self):
            for c, cond in self.totals:
                guarded(cond, c.wait_recv)

        def sent(self):
            for c, cond in self.totals:
                guarded(cond, c.wait_send)

    def guarded(cond, f):
        if cond is None:
            f()
        else:
            pl.when(cond)(f)

    near_conds = [cond for _, cond in near]
    at_end = (w == 0) | (w == N_WIDE - 1)
    by_end = (w == 1) | (w == N_WIDE - 2)
    inner = (w > 1) & (w < N_WIDE - 2)

    def near_group(moves, c):
        return Group(moves, [(back.at[c, pl.ds(0, n)], cond) for n, cond in ((112, inner), (88, by_end), (56, at_end))])

    tile = [slice(c * 128, c * 128 + 128) for c in range(TILES)]
    hop = {
        c: Group([(volume.at[:, :, tile[c]], xa.at[k, c], ring[k]) for k in range(3)], [(xa.at[:, c], None)])
        for c in range(TILES) if c not in Z_FIRST
    }
    raw = {c: Group([(volume.at[:, :, tile[c]], zv.at[c], across)], [(zv.at[c], None)]) for c in Z_FIRST}
    spread = {c: Group([(xo.at[c, k], xi.at[c, k], ring[k]) for k in range(3)], [(xi.at[c], None)]) for c in Z_FIRST}
    cross = {c: Group([(zs.at[c], zr.at[c], across)], [(zr.at[c], None)]) for c in range(TILES) if c not in Z_FIRST}
    rows_sent = {-1: (56, 32, 88), 1: (56, 32, 24), -2: (56, 24, 120), 2: (64, 24, 0)}
    halo = [
        near_group([(phase.at[c, pl.ds(rows_sent[d][0], rows_sent[d][1]), :], phase.at[c, pl.ds(rows_sent[d][2], rows_sent[d][1]), :],
                     (g, jnp.clip(w + d, 0, N_WIDE - 1))) for d, _ in near], c)
        for c in range(TILES)
    ]
    rows_back = {-1: (24, 32, 0), 1: (88, 32, 32), -2: (0, 24, 64), 2: (120, 24, 88)}
    ret = [
        near_group([(acc.at[c + 1, pl.ds(rows_back[d][0], rows_back[d][1]), :], back.at[c, pl.ds(rows_back[d][2], rows_back[d][1]), :],
                     (g, jnp.clip(w + d, 0, N_WIDE - 1))) for d, _ in near], c)
        for c in range(TILES)
    ]
    gcross = [Group([(pair_g.at[c, 0], pair_g.at[c, 1], across)], [(zr.at[c], None)]) for c in range(TILES)]
    ghop = [
        Group([(pair_g.at[c, h], ga.at[k, c, h], ring[k]) for h in range(2) for k in range(3)], [(ga.at[:, c], None)])
        for c in range(TILES)
    ]
    sums = [Group([(mbuf.at[s, groups[s][0]], mbuf.at[s, groups[s][0]], p) for p in groups[s][1]], [(mbuf.at[s, pl.ds(0, 7)], None)]) for s in range(3)]

    loads = [
        pltpu.make_async_copy(src, dst, load_sems.at[k])
        for k, (src, dst) in enumerate((
            (volume_in, volume), (probe_in, probe2.at[:, pl.ds(0, PATCH)]), (probe_in, probe2.at[:, pl.ds(PATCH, PATCH)]),
            (paths_in, paths), (steps_in, steps), (jitter_in, jitter), (measured_in, measured), (tables_in, tables),
        ))
    ]
    barrier = pltpu.get_barrier_semaphore()
    for _, members in groups:
        for p in members:
            pl.semaphore_signal(barrier, inc=1, device_id=p, device_id_type=MESH)
    for d, cond in near:
        @pl.when(cond)
        def _():
            pl.semaphore_signal(barrier, inc=1, device_id=(g, jnp.clip(w + d, 0, N_WIDE - 1)), device_id_type=MESH)

    for c in loads:
        c.start()
    for t in (0, TILES + 1):
        cosf[t] = jnp.zeros((FRAME, 128), F32)
        sinf[t] = jnp.zeros((FRAME, 128), F32)
    acc[...] = jnp.zeros(acc.shape, F32)
    err[...] = jnp.zeros(err.shape, F32)

    neighbours = sum(cond.astype(jnp.int32) for _, cond in near)
    loads[0].wait()
    with jax.named_scope("wait"):
        pl.semaphore_wait(barrier, 21 + neighbours)
    for c in Z_FIRST:
        raw[c].start()
    for c in hop:
        hop[c].start()
    for c in loads[1:]:
        c.wait()

    slabs = [g, x_down * 2 + zh, x_up * 2 + zh, x_far * 2 + zh]

    partner = g + 1 - 2 * zh

    def stage_b_across(c):
        raw[c].arrive()

        def both(angle):
            s = jnp.zeros((ROWS, 128), F32)
            for l in range(2):
                s = s + paths[angle, l, g] * volume[l, :, tile[c]] + paths[angle, l, partner] * zv[c, l]
            return s

        for k, x_ in enumerate((x_up, x_down, x_far)):
            xo[c, k] = both(x_ * 2 + zh)
            spread[c].start([k])
        phase[c, TOP : TOP + ROWS, :] = both(g)

    def stage_b(c):
        if c in Z_FIRST:
            return stage_b_across(c)
        hop[c].arrive()
        blocks = [(volume[l, :, tile[c]], xa[0, c, l], xa[1, c, l], xa[2, c, l]) for l in range(2)]

        def term(angle):
            s = jnp.zeros((ROWS, 128), F32)
            for l in range(2):
                for k in range(4):
                    s = s + paths[angle, l, slabs[k]] * blocks[l][k]
            return s

        zs[c] = term(g + 1 - 2 * zh)
        cross[c].start()
        phase[c, TOP : TOP + ROWS, :] = term(g)

    def stage_c(c):
        if c in Z_FIRST:
            spread[c].arrive()
            rest = xi[c, 0] + xi[c, 1] + xi[c, 2]
        else:
            cross[c].arrive()
            rest = zr[c]
        phase[c, TOP : TOP + ROWS, :] = phase[c, TOP : TOP + ROWS, :] + rest
        halo[c].start(conds=near_conds)

    first = TOP - ROWS * w

    def stage_d(c):
        halo[c].arrive()
        for r in range(0, FRAME, 24):
            row = lax.broadcasted_iota(jnp.int32, (24, 128), 0) + r
            inside = (row >= first) & (row < first + ROWS * N_WIDE)
            co, si = cos_sin(jnp.where(inside, phase[c, r : r + 24, :], 0.0))
            cosf[c + 1, r : r + 24, :] = jnp.where(inside, co, 0.0)
            sinf[c + 1, r : r + 24, :] = jnp.where(inside, si, 0.0)

    def masks(pair, p):
        j = 2 * pair + p
        jr = jitter[0, j]
        s = (24 if p else 88) + jitter[1, j]
        lane = lax.broadcasted_iota(jnp.int32, (CHUNK, PATCH), 1) >= s
        row = lax.broadcasted_iota(jnp.int32, (16, PATCH), 0) >= jr
        return j, jr, s, lane, row

    def put_rows(slot, p, c, a, b):
        at = slice(p * PATCH + c, p * PATCH + c + CHUNK)
        for k, x in enumerate((a, b)):
            hi, lo = halves(x)
            xs[slot, at, k * 128 : k * 128 + 128] = hi
            xs[slot, at, 256 + k * 128 : 256 + k * 128 + 128] = lo

    def right(slot, th, tl):
        x = xs[slot]
        return mm(jnp.concatenate([x, x[:, :256]], 1), jnp.concatenate([th, th, tl], 0))

    def to_cols(slot, u):
        for p in range(2):
            for k in range(2):
                for c in range(0, PATCH, CHUNK):
                    hi, lo = halves(u[p * PATCH + c : p * PATCH + c + CHUNK, k * 128 : k * 128 + 128])
                    vs[slot, k * PATCH + c : k * PATCH + c + CHUNK, p * 128 : p * 128 + 128] = hi
                    vs[slot, 256 + k * PATCH + c : 256 + k * PATCH + c + CHUNK, p * 128 : p * 128 + 128] = lo

    def left(slot, th, tl):
        v = vs[slot]
        return mm(jnp.concatenate([th, th, tl], 1), jnp.concatenate([v, v[:256]], 0))

    def waves(pair, slot):
        for p in range(2):
            j, jr, s, lane, row = masks(pair, p)
            t = pair + p
            for c in range(0, PATCH, CHUNK):
                def pick(ref):
                    a = ref[t, c : c + CHUNK, :]
                    b = ref[t + 1, c : c + CHUNK, :]
                    if c == 0:
                        a0 = jnp.where(row, a[:16], ref[t, PATCH:, :])
                        b0 = jnp.where(row, b[:16], ref[t + 1, PATCH:, :])
                        a = jnp.concatenate([a0, a[16:]], 0)
                        b = jnp.concatenate([b0, b[16:]], 0)
                    return jnp.where(lane, a, b)
                o_r, o_i = pick(cosf), pick(sinf)
                at = pl.ds(PATCH - jr + c, CHUNK)
                p_r = pltpu.roll(probe2[0, at, :], s, 1)
                p_i = pltpu.roll(probe2[1, at, :], s, 1)
                w_r = p_r * o_r - p_i * o_i
                w_i = p_r * o_i + p_i * o_r
                wave[slot, p, 0, c : c + CHUNK, :] = w_r
                wave[slot, p, 1, c : c + CHUNK, :] = w_i
                put_rows(slot, p, c, w_r, w_i)
    def pointwise(pair, slot, y):
        e = err[...]
        for p in range(2):
            j = 2 * pair + p
            for c in range(0, PATCH, CHUNK):
                f_r = y[c : c + CHUNK, p * 128 : p * 128 + 128]
                f_i = y[PATCH + c : PATCH + c + CHUNK, p * 128 : p * 128 + 128]
                m2 = f_r * f_r + f_i * f_i
                target = measured[j, c : c + CHUNK, :].astype(F32)
                d = jnp.sqrt(m2) - target
                d2 = d * d
                for k in range(0, CHUNK, 8):
                    e = e + d2[k : k + 8]
                ratio = target * lax.rsqrt(jnp.maximum(m2, 0.0625))
                put_rows(2 + slot, p, c, ratio * f_r, ratio * f_i)
        err[...] = e
    def accumulate(pair, slot, y):
        for p in range(2):
            j, jr, s, lane, row = masks(pair, p)
            t = pair + p
            for c in range(0, PATCH, CHUNK):
                b_r = y[c : c + CHUNK, p * 128 : p * 128 + 128]
                b_i = y[PATCH + c : PATCH + c + CHUNK, p * 128 : p * 128 + 128]
                g = wave[slot, p, 0, c : c + CHUNK, :] * b_i - wave[slot, p, 1, c : c + CHUNK, :] * b_r
                for tile, part in ((t, jnp.where(lane, g, 0.0)), (t + 1, jnp.where(lane, 0.0, g))):
                    if c == 0:
                        acc[tile, PATCH:, :] += jnp.where(row, 0.0, part[:16])
                        part = jnp.concatenate([jnp.where(row, part[:16], 0.0), part[16:]], 0)
                    acc[tile, c : c + CHUNK, :] += part

    def stage_e(i):
        t1h, t1l, t2h, t2l = (tables[k] for k in range(4))
        ahead, behind = i < PCOLS // 2, i > 0
        if behind:
            u2 = right(2 + (i - 1) % 2, t2h, t2l)
        if ahead:
            waves(i, i % 2)
            u1 = right(i % 2, t1h, t1l)
        if behind:
            to_cols(1, u2)
            y2 = left(1, t1h, t1l)
        if ahead:
            to_cols(0, u1)
            y1 = left(0, t2h, t2l)
        if behind:
            accumulate(i - 1, (i - 1) % 2, y2)
        if ahead:
            pointwise(i, i % 2, y1)

    def stage_f(c):
        ret[c].start(conds=near_conds)

    def stage_g(c):
        pair_g[c, 0] = acc[c + 1, TOP : TOP + ROWS, :]
        ret[c].arrive()
        for k, (d, cond) in enumerate(near):
            ok = {1: w >= 1, -1: w < N_WIDE - 1, 2: w >= 2, -2: w < N_WIDE - 2}[d]
            lo, n, at = {-1: (0, 32, 0), 1: (0, 32, 32), -2: (8, 24, 64), 2: (0, 24, 88)}[d]

            @pl.when(ok)
            def _():
                pair_g[c, 0, lo : lo + n, :] = pair_g[c, 0, lo : lo + n, :] + back[c, at : at + n, :]

        gcross[c].start()
        ghop[c].start((0, 1, 2))

    def stage_h(c):
        gcross[c].arrive()
        ghop[c].start((3, 4, 5))

    angles = [g, g + 1 - 2 * zh, x_down * 2 + zh, x_down * 2 + 1 - zh, x_up * 2 + zh, x_up * 2 + 1 - zh, x_far * 2 + zh, x_far * 2 + 1 - zh]

    def stage_j(c):
        ghop[c].arrive()
        grads = [pair_g[c, 0], pair_g[c, 1], *(ga[k, c, h] for k in range(3) for h in range(2))]
        for l in range(2):
            s = jnp.zeros((ROWS, 128), F32)
            for a, gr in zip(angles, grads):
                s = s + (steps[a] * paths[a, l, g]) * gr
            out[l, :, tile[c]] = s

    def misfit_send(s, value):
        mbuf[s, pl.ds(groups[s][0], 1)] = value[None]
        sums[s].start()

    def misfit_take(s):
        sums[s].arrive()
        v = mbuf[s, 0]
        for k in range(1, 8):
            v = v + mbuf[s, k]
        return v

    def stage_m(c):
        value = misfit_take(c - 1) if c else jnp.sum(err[...], 0, keepdims=True)
        if c < 3:
            misfit_send(c, value)
        else:
            total[...] = jnp.full((8, 128), jnp.sum(value), F32)

    stages = dict(zip("BCDEFGHJM", (stage_b, stage_c, stage_d, stage_e, stage_f, stage_g, stage_h, stage_j, stage_m)))
    def drop(count):
        for c in pending[:count]:
            c.sent()
        del pending[:count]

    plan = order()
    tail = plan.index(("F", TILES - 1)) + 1
    for at, (name, c) in enumerate(plan):
        if at >= tail and len(pending) > 9:
            drop(3)
        with jax.named_scope(f"{name}{c}"):
            stages[name](c)
    with jax.named_scope("end"):
        drop(len(pending))


STEP = 1.0
Z_FIRST = (1, 2)


def order():
    tiles = range(TILES)
    due, ready, turn = [], [], {True: 0, False: 0}
    for c in tiles:
        z_first = c in Z_FIRST
        k = turn[z_first]
        turn[z_first] += 1
        begin = 6.9 + 1.4 * k if z_first else 2.2 + 1.4 * k
        joined = begin + (2.7 if z_first else 6.6)
        due += [(begin, "B", c), (joined, "C", c), (joined + 3.7, "D", c)]
        ready.append(joined + 3.7)
    done, now = [], 0.0
    for i in range(TILES + 1):
        now = max(now, max(ready[: i + 2]) + 0.01)
        due.append((now, "E", i))
        now += STEP
        done.append(now - 0.01)
    for c in tiles:
        t = done[min(c + 2, TILES)]
        due += [(t, "F", c), (t + 3.8 - 0.15 * c, "G", c), (t + 9.3 - 0.15 * c, "H", c), (t + 13.5 - 0.15 * c, "J", c)]
    due += [(done[TILES - 1] - 0.001 + t, "M", c) for c, t in enumerate((0.0, 4.6, 10.4, 15.0))]
    return [(name, c) for _, name, c in sorted(due)]


def fused(volume, paths, steps, probe, measured, jitter):
    vm = pl.BlockSpec(memory_space=pltpu.VMEM)
    hbm = pl.BlockSpec(memory_space=pl.ANY)
    copies = TILES * 6 + 3
    grid = pltpu.VMEM((TILES + 2, FRAME, 128), F32)
    return pl.pallas_call(
        fused_kernel,
        out_shape=(pltpu.VMEM((2, ROWS, COLS), F32), pltpu.VMEM((8, 128), F32)),
        in_specs=[hbm] * 7,
        out_specs=(vm, vm),
        scratch_shapes=[
            pltpu.VMEM((2, ROWS, COLS), F32),
            pltpu.VMEM((PCOLS, PATCH, PATCH), BF16),
            pltpu.VMEM((4, 2 * PATCH, 2 * PATCH), BF16),
            pltpu.SMEM((8, 2, 8), F32),
            pltpu.SMEM((8,), F32),
            pltpu.SMEM((2, PCOLS), jnp.int32),
            pltpu.SemaphoreType.DMA((8,)),
            pltpu.VMEM((3, TILES, 2, ROWS, 128), F32),
            pltpu.VMEM((TILES, 2, ROWS, 128), F32),
            pltpu.VMEM((TILES, 3, ROWS, 128), F32),
            pltpu.VMEM((TILES, 3, ROWS, 128), F32),
            pltpu.VMEM((TILES, ROWS, 128), F32),
            pltpu.VMEM((TILES, ROWS, 128), F32),
            pltpu.VMEM((TILES, FRAME, 128), F32),
            grid, grid, grid,
            pltpu.VMEM((TILES, 112, 128), F32),
            pltpu.VMEM((TILES, 2, ROWS, 128), F32),
            pltpu.VMEM((3, TILES, 2, ROWS, 128), F32),
            pltpu.VMEM((2, 2 * PATCH, PATCH), F32),
            pltpu.VMEM((2, 2, 2, PATCH, PATCH), F32),
            pltpu.VMEM((4, 2 * PATCH, 512), BF16),
            pltpu.VMEM((2, 512, 2 * PATCH), BF16),
            pltpu.VMEM((8, 128), F32),
            pltpu.VMEM((3, 8, 1, 128), F32),
            pltpu.SemaphoreType.DMA((copies,)),
            pltpu.SemaphoreType.DMA((copies,)),
        ],
        compiler_params=pltpu.CompilerParams(collective_id=0, has_side_effects=True),
        name="fused",
    )(volume, paths, steps, probe, measured, jitter, jnp.asarray(dft_tables()))


def body(volume, path_lengths, probe, measured, jitter, step_sizes):
    paths = jnp.transpose(path_lengths, (0, 2, 1))
    update, total = fused(volume[0], paths, step_sizes, probe, measured[0, 0], jitter[:, 0, 0])
    return volume - update[None], total[0, 0]


def solution(mesh):
    in_specs = (
        P("blk", None, "wide", None),
        P(),
        P(),
        P("blk", "wide", None, None, None),
        P(None, "blk", "wide", None),
        P(),
    )
    out_specs = (P("blk", None, "wide", None), P())
    return jax.shard_map(body, mesh=mesh, in_specs=in_specs, out_specs=out_specs, check_vma=False)
```
